128 devices in a mesh: mem: 4 (over y_lo, core), lat: 4 (over z), lon: 8 (over y_hi, x).
Axes of the slice: x: 4, y: 4 (y_hi: 2, y_lo: 2; y = y_hi * 2 + y_lo), z: 4, core: 2. Of those that a mesh axis runs over, the one named last changes fastest.
Arguments:
- fields: bfloat16 [4, 2, 96, 384, 512], P('mem', None, 'lat', 'lon'), may hold values from -6 to 6
- region: int32 [96, 384], P('lat', 'lon'), may hold values from 0 to 2
- gain_attn: float32 [512], replicated, may hold values from 0.1 to 1.9
- w_qkv: bfloat16 [512, 1536], P(None, ('mem', 'lat', 'lon')), may hold values from -1 to 1
- w_proj: bfloat16 [512, 512], P(None, ('mem', 'lat', 'lon')), may hold values from -0.25 to 0.25
- gain_mlp: float32 [512], replicated, may hold values from 0.1 to 1.9
- w_up: bfloat16 [512, 2048], P(None, ('mem', 'lat', 'lon')), may hold values from -0.25 to 0.25
- w_down: bfloat16 [2048, 512], P(None, ('mem', 'lat', 'lon')), may hold values from -0.125 to 0.125
Outputs:
- updated: bfloat16 [4, 2, 96, 384, 512], P('mem', None, 'lat', 'lon')
The draws below stay inside these ranges and needn't reach their ends.
All inputs are finite; a program needn't handle non-finite values.
Results may differ from the reference program's by a relative error of at most 0.011.
Values may be sent and summed in bfloat16 or wider, within the bound.
A program may use at most 192 MiB of HBM per device.

```python
import jax
import jax.numpy as jnp
from jax import lax

D = 512
HEADS = 16
FF = 2048
HDIM = 32
WLAT = 6
WLON = 12
LEVELS = 2
SH = 3
SL = 6
MEMBERS = 4
NLAT = 96
NLON = 384


def draw_w_qkv(key, part):
    first = jax.random.fold_in(key, 11)
    drawn = jnp.clip(jax.random.normal(first, (D, 3 * D), jnp.float32), -6.0, 6.0) / D ** 0.5
    return drawn.astype(jnp.bfloat16)


def with_ends(array, key, least, top_value):
    shape = array.shape
    index_at = [jax.random.randint(jax.random.fold_in(key, axis), (), 0, shape[axis]) for axis in range(len(shape))]
    array = array.at[tuple(index_at)].set(least)
    longest = shape.index(max(shape))
    index_at[longest] = (index_at[longest] + 1) % shape[longest]
    return array.at[tuple(index_at)].set(top_value)


def levels(own_key, dims, split, low, largest):
    factor_of = 1.0
    for axis_at, blocks in split:
        heights = jax.random.uniform(jax.random.fold_in(jax.random.fold_in(own_key, 6), axis_at), (blocks,), jnp.float32, low / len(split), largest / len(split))
        factor_of = factor_of * jnp.repeat(jnp.exp(heights), dims[axis_at] // blocks).reshape((-1,) + (1,) * (len(dims) - 1 - axis_at))
    return factor_of


def scatter_about(rng, dims, deviation, most, split=(), held_as=jnp.bfloat16):
    drawn = deviation * jax.random.normal(rng, dims, jnp.float32)
    if split:
        drawn = drawn * levels(rng, dims, split, -0.22, 0.18)
    return jnp.clip(drawn, -most, most).astype(held_as)


def setup_inputs(seed: int = 0) -> dict:
    splits = jax.random.split(jax.random.key(seed), 9)
    fields = scatter_about(splits[0], (MEMBERS, LEVELS, NLAT, NLON, D), 1.0, 6.0, ((0, 4), (2, 4), (3, 8)))
    region = with_ends(jax.random.randint(splits[1], (NLAT, NLON), 0, 3), jax.random.fold_in(splits[1], 1), 0, 2).astype(jnp.int32)
    gain_attn = jnp.clip(1.0 + 0.18 * jax.random.normal(splits[2], (D,), jnp.float32), 0.1, 1.9)
    w_qkv = draw_w_qkv(jax.random.fold_in(splits[8], 71), 0)
    w_proj = scatter_about(splits[4], (D, D), D ** -0.5, 0.25, ((1, 128),))
    gain_mlp = jnp.clip(1.0 + 0.18 * jax.random.normal(splits[5], (D,), jnp.float32), 0.1, 1.9)
    w_up = scatter_about(splits[6], (D, FF), D ** -0.5, 0.25, ((1, 128),))
    w_down = scatter_about(splits[7], (FF, D), FF ** -0.5, 0.125, ((1, 128),))
    return dict(fields=fields, region=region, gain_attn=gain_attn, w_qkv=w_qkv, w_proj=w_proj, gain_mlp=gain_mlp, w_up=w_up, w_down=w_down)


eps = 1e-05

def layer_norm(values, gain_vec):
    values = values.astype(jnp.float32)
    average = lax.optimization_barrier(jnp.mean(values, axis=-1, keepdims=True))
    centred = values - average
    variance = lax.optimization_barrier(jnp.mean(centred * centred, axis=-1, keepdims=True))
    return (centred * lax.rsqrt(variance + eps) * gain_vec).astype(jnp.bfloat16)

def to_windows(arr):
    chans = arr.shape[-1]
    arr = arr.reshape(LEVELS, NLAT // WLAT, WLAT, NLON // WLON, WLON, chans)
    arr = arr.transpose(1, 3, 0, 2, 4, 5)
    return arr.reshape(NLAT // WLAT, NLON // WLON, LEVELS * WLAT * WLON, chans)

def reference(fields, region, gain_attn, w_qkv, w_proj, gain_mlp, w_up, w_down):
    scale = 1.0 / HDIM ** 0.5
    win_tok = LEVELS * WLAT * WLON
    shifted_ids = jnp.roll(region, (-SH, -SL), axis=(0, 1)).astype(jnp.int32)
    north = ((jnp.arange(NLAT) + SH) % NLAT < SH).astype(jnp.int32)
    ids_win = to_windows(jnp.broadcast_to(shifted_ids[None, :, :, None], (LEVELS, NLAT, NLON, 1)))[..., 0]
    north_win = to_windows(jnp.broadcast_to(north[None, :, None, None], (LEVELS, NLAT, NLON, 1)))[..., 0]

    def band_fn(args):
        tokens, ids_band, north_band = args
        count = tokens.shape[0]
        qkv_all = jnp.dot(tokens.reshape(-1, D), w_qkv, preferred_element_type=jnp.float32).astype(jnp.bfloat16)
        qkv_all = qkv_all.reshape(count, win_tok, 3, HEADS, HDIM).astype(jnp.float32)
        queries = qkv_all[:, :, 0]
        keys_in = qkv_all[:, :, 1]
        values_in = qkv_all[:, :, 2]
        scores = jnp.einsum('wqhd,wkhd->whqk', queries, keys_in) * scale
        allow = (ids_band[:, :, None] == ids_band[:, None, :]) & (north_band[:, :, None] == north_band[:, None, :])
        scores = jnp.where(allow[:, None], scores, -1000000000.0)
        attn_probs = jax.nn.softmax(scores, axis=-1).astype(jnp.bfloat16)
        mixed_heads = jnp.einsum('whqk,wkhd->wqhd', attn_probs.astype(jnp.float32), values_in).astype(jnp.bfloat16)
        mixed_heads = mixed_heads.reshape(count * win_tok, D)
        projected = jnp.dot(mixed_heads, w_proj, preferred_element_type=jnp.float32).astype(jnp.bfloat16)
        return projected.reshape(count, win_tok, D)

    def one_member(member):
        normed = layer_norm(member, gain_attn)
        shifted = jnp.roll(normed, (-SH, -SL), axis=(1, 2))
        out_win = lax.map(band_fn, (to_windows(shifted), ids_win, north_win))
        out_win = out_win.reshape(NLAT // WLAT, NLON // WLON, LEVELS, WLAT, WLON, D)
        attn_out = out_win.transpose(2, 0, 3, 1, 4, 5).reshape(LEVELS, NLAT, NLON, D)
        attn_out = jnp.roll(attn_out, (SH, SL), axis=(1, 2))
        resid = (member.astype(jnp.float32) + attn_out.astype(jnp.float32)).astype(jnp.bfloat16)
        normed2 = layer_norm(resid, gain_mlp).reshape(-1, D)
        hidden = jax.nn.gelu(jnp.dot(normed2, w_up, preferred_element_type=jnp.float32), approximate=False).astype(jnp.bfloat16)
        delta = jnp.dot(hidden, w_down, preferred_element_type=jnp.float32).reshape(LEVELS, NLAT, NLON, D)
        return (resid.astype(jnp.float32) + delta).astype(jnp.bfloat16)
    return lax.map(one_member, fields)
```

```python
import functools

import jax
import jax.numpy as jnp
from jax import lax
from jax.experimental import pallas as pl
from jax.experimental.pallas import tpu as pltpu
from jax.sharding import PartitionSpec as P

D = 512
FF = 2048
HDIM = 32
WLAT = 6
WLON = 12
WTOK = 144
SH = 3
SL = 6
NLAT_ALL = 96
QSCALE = 1.4426950408889634 / HDIM**0.5
NEG = -1e30
EPS = 1e-05
MESH = pl.DeviceIdType.MESH
BF = jnp.bfloat16
F32 = jnp.float32

S_P1 = 0
S_P2 = 3
S_UP = 6
S_DN = 10
S_FW = 14
S_CO = 18
S_ALL = 34


def nt(a, b):
    return lax.dot_general(a, b, (((1,), (1,)), ((), ())), preferred_element_type=F32)


def nn(a, b):
    return lax.dot_general(a, b, (((1,), (0,)), ((), ())), preferred_element_type=F32)


def norm(x, gain):
    x = x.astype(F32)
    mean = jnp.mean(x, axis=-1, keepdims=True)
    cen = x - mean
    var = jnp.mean(cen * cen, axis=-1, keepdims=True)
    return (cen * lax.rsqrt(var + EPS) * gain).astype(BF)


def kernel(
    shard,
    fields,
    region,
    gain_a,
    gain_m,
    toks,
    out,
    gat,
    fx,
    reg,
    w_qkv,
    w_p,
    w_d,
    xb,
    q_s,
    k_s,
    vt_s,
    mt,
    mix,
    ox,
    ic,
    km_mask,
    tq_mask,
    to_mask,
    ob,
    send,
    recv,
    loc,
    hsend,
    hrecv,
    osem,
):
    mem = lax.axis_index("mem")
    lat = lax.axis_index("lat")
    lon = lax.axis_index("lon")
    core = mem % 2
    y_lo = mem // 2
    y_hi = lon // 4
    x0 = lon % 4
    y0 = y_hi * 2 + y_lo
    pos = (x0, y0, lat)

    def dev(x, y, z, c):
        return ((y % 2) * 2 + c, z, (y // 2) * 4 + x)

    def moved(axis, dist, c=None):
        p = list(pos)
        p[axis] = (p[axis] + dist) % 4
        return dev(*p, core if c is None else c)

    sibling = dev(*pos, 1 - core)
    lat_b, lat_f = (lat + 3) % 4, (lat + 1) % 4
    lon_b, lon_f = (lon + 7) % 8, (lon + 1) % 8

    bar = pltpu.get_barrier_semaphore()
    peers = [moved(a, d) for a in range(3) for d in (1, 2, 3)] + [sibling]
    peers += [(mem, lat, lon_b), (mem, lat, lon_f), (mem, lat_b, lon_b), (mem, lat_f, lon_f)]
    for d in peers:
        pl.semaphore_signal(bar, inc=1, device_id=d, device_id_type=MESH)

    own = pltpu.make_async_copy(fields, fx.at[:, pl.ds(0, 24), pl.ds(0, 48)], loc.at[3])
    own.start()
    own_reg = pltpu.make_async_copy(region, reg.at[0, pl.ds(0, 24)], loc.at[4])
    own_reg.start()

    def chip(x, y, z, c):
        return (y % 2, c, z, y // 2, x)

    locals_ = []
    for p in range(3):
        cp = pltpu.make_async_copy(shard.at[p], gat.at[(p, *chip(*pos, core))], loc.at[p])
        cp.start()
        locals_.append(cp)

    pl.semaphore_wait(bar, len(peers))

    def remote(src, dst, s, r, d):
        cp = pltpu.make_async_remote_copy(
            src_ref=src, dst_ref=dst, send_sem=s, recv_sem=r, device_id=d, device_id_type=MESH
        )
        cp.start()
        return cp

    pend = []

    def blk(p, bval, cval, c):
        a, b, cc = p, (p + 1) % 3, (p + 2) % 3
        v = [None, None, None]
        v[b], v[cc] = bval, cval
        x, y, z = v
        full = pl.ds(0, 4)
        if y is None:
            yl, yh = pl.ds(0, 2), pl.ds(0, 2)
        else:
            yl, yh = y % 2, y // 2
        x = full if x is None else x
        z = full if z is None else z
        return gat.at[p, yl, c, z, yh, x]

    ph1 = {}
    for p in range(3):
        for i, d in enumerate((1, 3, 2)):
            here = gat.at[(p, *chip(*pos, core))]
            ph1[p, i] = remote(
                shard.at[p], here, send.at[p, S_P1 + i], recv.at[p, S_P1 + i], moved(p, d)
            )
            pend.append(ph1[p, i])

    halos = []
    fsl = (
        (fields.at[:, pl.ds(0, 3)], fx.at[:, pl.ds(24, 3), pl.ds(0, 48)], (mem, lat_b, lon)),
        (fields.at[:, :, pl.ds(0, 8)], fx.at[:, pl.ds(0, 24), pl.ds(48, 8)], (mem, lat, lon_b)),
        (
            fields.at[:, pl.ds(0, 3), pl.ds(0, 8)],
            fx.at[:, pl.ds(24, 3), pl.ds(48, 8)],
            (mem, lat_b, lon_b),
        ),
        (region, reg.at[0, pl.ds(24, 24)], (mem, lat_b, lon)),
        (region, reg.at[1, pl.ds(0, 24)], (mem, lat, lon_b)),
        (region, reg.at[1, pl.ds(24, 24)], (mem, lat_b, lon_b)),
    )
    for i, (s, t, d) in enumerate(fsl):
        halos.append(remote(s, t, hsend.at[i], hrecv.at[i], d))

    for cp in locals_:
        cp.wait()

    b0 = [pos[(p + 1) % 3] for p in range(3)]
    c0 = [pos[(p + 2) % 3] for p in range(3)]
    ph2, up, down, fwd, swap = {}, {}, {}, {}, {}
    dists = (0, 3, 1, 2)

    def to_core(p, slot, bval, cval):
        r = blk(p, bval, cval, core)
        swap[p, slot] = remote(r, r, send.at[p, S_CO + slot], recv.at[p, S_CO + slot], sibling)
        pend.append(swap[p, slot])

    def to_last(p, i):
        bval = (b0[p] + dists[i]) % 4
        r = blk(p, bval, c0[p], core)
        ax = (p + 2) % 3
        up[p, i] = remote(r, r, send.at[p, S_UP + i], recv.at[p, S_UP + i], moved(ax, 1))
        down[p, i] = remote(r, r, send.at[p, S_DN + i], recv.at[p, S_DN + i], moved(ax, 3))
        pend.extend((up[p, i], down[p, i]))
        to_core(p, i, bval, c0[p])

    for p in range(3):
        for i in range(3):
            ph1[p, i].wait_recv()
        r = blk(p, b0[p], c0[p], core)
        for i, d in enumerate((1, 3, 2)):
            ph2[p, i] = remote(
                r, r, send.at[p, S_P2 + i], recv.at[p, S_P2 + i], moved((p + 1) % 3, d)
            )
            pend.append(ph2[p, i])
        to_last(p, 0)
    for i in range(3):
        for p in range(3):
            ph2[p, i].wait_recv()
            to_last(p, i + 1)

    lane = lax.broadcasted_iota(jnp.int32, (WTOK, 128), 1)
    for h in range(4):
        km_mask[h] = jnp.where((lane >> 5) == h, 1.0, 0.0).astype(BF)
    tr = lax.broadcasted_iota(jnp.int32, (128, 256), 0)
    tl = lax.broadcasted_iota(jnp.int32, (128, 256), 1)
    tq_mask[...] = jnp.where((tr >> 4) == (tl >> 5), 1.0, 0.0).astype(BF)
    tr = lax.broadcasted_iota(jnp.int32, (256, 128), 0)
    tl = lax.broadcasted_iota(jnp.int32, (256, 128), 1)
    to_mask[...] = jnp.where((tr >> 5) == (tl >> 4), 1.0, 0.0)

    is_up = core == 0
    for i in range(4):
        for p in range(3):
            bval = (b0[p] + dists[i]) % 4
            ax = (p + 2) % 3
            up[p, i].wait_recv()
            down[p, i].wait_recv()
            cval = jnp.where(is_up, (c0[p] + 3) % 4, (c0[p] + 1) % 4)
            step = jnp.where(is_up, 1, 3)
            r = blk(p, bval, cval, core)
            fwd[p, i] = remote(
                r, r, send.at[p, S_FW + i], recv.at[p, S_FW + i], moved(ax, step)
            )
            pend.append(fwd[p, i])
            to_core(p, 4 + i, bval, (c0[p] + 3) % 4)
            to_core(p, 8 + i, bval, (c0[p] + 1) % 4)
    for i in range(4):
        for p in range(3):
            bval = (b0[p] + dists[i]) % 4
            fwd[p, i].wait_recv()
            to_core(p, 12 + i, bval, (c0[p] + 2) % 4)
    for p in range(3):
        for i in range(16):
            swap[p, i].wait_recv()
    own.wait()
    own_reg.wait()
    for h in halos:
        h.wait_recv()

    @pl.loop(0, 32)
    def _(g):
        at = (g // 16, (g // 8) % 2, (g // 2) % 4, g % 2)
        v = gat[(0, *at)]
        w_qkv[pl.ds(pl.multiple_of(g * 48, 16), 48), :] = jnp.concatenate(
            [v[i, 0:12] for i in range(4)], axis=0
        )
        w_p[pl.ds(pl.multiple_of(g * 16, 16), 16), :] = jnp.concatenate(
            [v[i, 12:16] for i in range(4)], axis=0
        )
        u = gat[(2, *at)]
        for k in range(4):
            w_d[pl.ds(pl.multiple_of(g * 16, 16), 16), 512 * k : 512 * k + 512] = jnp.concatenate(
                [u[i, 4 * k : 4 * k + 4] for i in range(4)], axis=0
            )

    @pl.loop(0, 4)
    def _(b):
        for w in range(4):
            pieces = [
                fx[l, 6 * b + SH + i, WLON * w + SL : WLON * w + SL + WLON, :]
                for l in range(2)
                for i in range(WLAT)
            ]
            xw = norm(jnp.concatenate(pieces, axis=0), gain_a[...])
            xb[WTOK * w : WTOK * w + WTOK, :] = xw
        rows = pl.ds(pl.multiple_of(b * 576, 16), 576)
        for n in range(2):
            cols = slice(256 * n, 256 * n + 256)
            q = nt(xb[...], w_qkv[256 * n : 256 * n + 256, :])
            q_s[rows, cols] = (q * QSCALE).astype(BF)
            k = nt(xb[...], w_qkv[512 + 256 * n : 512 + 256 * n + 256, :])
            k_s[rows, cols] = k.astype(BF)
        for w in range(4):
            vt = nt(w_qkv[1024:1536, :], xb[WTOK * w : WTOK * w + WTOK, :])
            vt_s[b * 4 + w] = vt.astype(BF)

    def window(b, w):
        win = b * 4 + w
        rows = pl.ds(pl.multiple_of(win * WTOK, 16), WTOK)
        row = toks[0] + (6 * b + SH)
        col = toks[1] + (WLON * w + SL)
        l48 = lax.broadcasted_iota(jnp.int32, (WTOK, 48), 1)
        sel = jnp.where(l48 == row, 1.0, 0.0).astype(BF)
        near = nn(sel, reg[0].astype(F32).astype(BF))
        far = nn(sel, reg[1].astype(F32).astype(BF))
        ids = jnp.sum(
            jnp.where(l48 == col, near, 0.0) + jnp.where(l48 + 48 == col, far, 0.0),
            axis=1,
            keepdims=True,
        )
        glob = lat * 24 + row
        glob = jnp.where(glob >= NLAT_ALL, glob - NLAT_ALL, glob)
        code = ids * 2.0 + jnp.where(glob < SH, 1.0, 0.0)
        hot = jnp.where(code == lane.astype(F32), 1.0, 0.0).astype(BF)
        bias_m = (nt(hot, hot[0:128]) - 1.0) * (-NEG)
        bias_t = (nt(hot, jnp.concatenate([hot[128:144]] * 8, axis=0)) - 1.0) * (-NEG)

        def softmax(s):
            m = jnp.max(s, axis=0, keepdims=True)
            e = jnp.exp2(s - m)
            return e.astype(BF), 1.0 / jnp.sum(e, axis=0, keepdims=True)

        for g in range(2):
            for s in range(2):
                at = 256 * g + 128 * s
                k4 = k_s[rows, at : at + 128]
                q4 = q_s[pl.ds(pl.multiple_of(win * WTOK, 16), 128), at : at + 128]
                for h in range(4):
                    e, inv = softmax(nt(k4 * km_mask[h], q4) + bias_m)
                    o = nn(vt_s[win, at + 32 * h : at + 32 * h + 32, :], e)
                    mt[at + 32 * h : at + 32 * h + 32, :] = (o * inv).astype(BF)
            at = 256 * g
            qt = q_s[pl.ds(pl.multiple_of(win * WTOK + 128, 16), 16), at : at + 256]
            qt = jnp.concatenate([qt] * 8, axis=0) * tq_mask[...]
            e, inv = softmax(nt(k_s[rows, at : at + 256], qt) + bias_t)
            o = nn(vt_s[win, at : at + 256, :], e)
            o = (o * inv * to_mask[...]).astype(BF).T
            acc = o[0:16]
            for h in range(1, 8):
                acc = acc + o[16 * h : 16 * h + 16]
            mix[pl.ds(pl.multiple_of(w * WTOK + 128, 16), 16), at : at + 256] = acc
        mix[pl.ds(pl.multiple_of(w * WTOK, 16), 128), :] = mt[...].T

    zeros = jnp.zeros((8, D), BF)

    @pl.loop(0, 4)
    def _(b):
        @pl.loop(0, 4)
        def _(w):
            window(b, w)

        ao = nt(mix[...], w_p[...]).astype(BF)
        for l in range(2):
            for i in range(WLAT):
                at = 72 * l + 12 * i
                pieces = [ao[WTOK * w + at : WTOK * w + at + 12] for w in range(4)]
                ox[l, 6 * b + SH + i] = jnp.concatenate(
                    [zeros[0:6], *pieces, zeros[0:2]], axis=0
                )

    backs = []
    bsl = (
        (ox.at[:, pl.ds(3, 21), pl.ds(48, 8)], ic.at[:, pl.ds(3, 21)], (mem, lat, lon_f)),
        (ox.at[:, pl.ds(24, 3), pl.ds(0, 48)], ox.at[:, pl.ds(0, 3), pl.ds(0, 48)], (mem, lat_f, lon)),
        (ox.at[:, pl.ds(24, 3), pl.ds(48, 8)], ic.at[:, pl.ds(0, 3)], (mem, lat_f, lon_f)),
    )
    for i, (s, t, d) in enumerate(bsl):
        backs.append(remote(s, t, hsend.at[6 + i], hrecv.at[6 + i], d))
    for cp in backs:
        cp.wait_recv()

    first = lax.broadcasted_iota(jnp.int32, (12, 8, D), 1) < SL

    outs = []
    for t in range(4):
        l, r = t // 2, 12 * (t % 2)
        att = ox[l, r : r + 12, 0:48, :].astype(F32)
        head = jnp.where(first, ic[l, r : r + 12].astype(F32), att[:, 0:8])
        att = jnp.concatenate([head, att[:, 8:48]], axis=1)
        res = (fx[l, r : r + 12, 0:48, :].astype(F32) + att).astype(BF).reshape(576, D)
        xb[...] = norm(res, gain_m[...])
        acc = res.astype(F32)
        for k in range(4):
            pre = nt(xb[...], gat[1, k // 2, k % 2].reshape(512, D))
            hid = (0.5 * pre * (1.0 + lax.erf(pre * 0.7071067811865476))).astype(BF)
            acc = acc + nt(hid, w_d[:, 512 * k : 512 * k + 512])
        ob[t] = acc.astype(BF).reshape(12, 48, D)
        cp = pltpu.make_async_copy(ob.at[t], out.at[l, pl.ds(r, 12)], osem.at[t])
        cp.start()
        outs.append(cp)

    for cp in pend + halos + backs:
        cp.wait_send()
    for cp in outs:
        cp.wait()


def body(fields, region, gain_attn, w_qkv, w_proj, gain_mlp, w_up, w_down):
    down = w_down.T.reshape(4, 4, D).transpose(1, 0, 2).reshape(16, D)
    shard = jnp.stack([jnp.concatenate([w_qkv.T, w_proj.T], axis=0), w_up.T, down])
    tok = jnp.arange(WTOK, dtype=jnp.int32)
    toks = jnp.stack([(tok // WLON) % WLAT, tok % WLON]).reshape(2, WTOK, 1)
    vm = pl.BlockSpec(memory_space=pltpu.VMEM)
    hbm = pl.BlockSpec(memory_space=pl.ANY)
    dma = pltpu.SemaphoreType.DMA
    out = pl.pallas_call(
        kernel,
        out_shape=jax.ShapeDtypeStruct((2, 24, 48, D), BF),
        in_specs=[hbm, hbm, hbm, vm, vm, vm],
        out_specs=hbm,
        scratch_shapes=[
            pltpu.VMEM((3, 2, 2, 4, 2, 4, 16, D), BF),
            pltpu.VMEM((2, 27, 56, D), BF),
            pltpu.VMEM((2, 48, 48), jnp.int32),
            pltpu.VMEM((3 * D, D), BF),
            pltpu.VMEM((D, D), BF),
            pltpu.VMEM((D, FF), BF),
            pltpu.VMEM((576, D), BF),
            pltpu.VMEM((2304, D), BF),
            pltpu.VMEM((2304, D), BF),
            pltpu.VMEM((16, D, WTOK), BF),
            pltpu.VMEM((D, 128), BF),
            pltpu.VMEM((576, D), BF),
            pltpu.VMEM((2, 27, 56, D), BF),
            pltpu.VMEM((2, 24, 8, D), BF),
            pltpu.VMEM((4, WTOK, 128), BF),
            pltpu.VMEM((128, 256), BF),
            pltpu.VMEM((256, 128), F32),
            pltpu.VMEM((4, 12, 48, D), BF),
            dma((3, S_ALL)),
            dma((3, S_ALL)),
            dma((5,)),
            dma((9,)),
            dma((9,)),
            dma((4,)),
        ],
        compiler_params=pltpu.CompilerParams(
            collective_id=0, has_side_effects=True, vmem_limit_bytes=66 * 2**20 - 2**21
        ),
        name="block",
    )(shard, fields[0], region, gain_attn.reshape(1, D), gain_mlp.reshape(1, D), toks)
    return out[None]


def solution(mesh):
    in_specs = (
        P("mem", None, "lat", "lon", None),
        P("lat", "lon"),
        P(),
        P(None, ("mem", "lat", "lon")),
        P(None, ("mem", "lat", "lon")),
        P(),
        P(None, ("mem", "lat", "lon")),
        P(None, ("mem", "lat", "lon")),
    )
    out_specs = P("mem", None, "lat", "lon", None)
    return jax.shard_map(body, mesh=mesh, in_specs=in_specs, out_specs=out_specs, check_vma=False)
```

```python
import functools

import jax
import jax.numpy as jnp
from jax import lax
from jax.experimental import pallas as pl
from jax.experimental.pallas import tpu as pltpu
from jax.sharding import PartitionSpec as P

D = 512
FF = 2048
HDIM = 32
WLAT = 6
WLON = 12
WTOK = 144
SH = 3
SL = 6
NLAT_ALL = 96
QSCALE = 1.4426950408889634 / HDIM**0.5
NEG = -1e30
EPS = 1e-05
MESH = pl.DeviceIdType.MESH
BF = jnp.bfloat16
F32 = jnp.float32

S_P1 = 0
S_P2 = 3
S_UP = 6
S_DN = 10
S_FW = 14
S_CO = 18
S_ALL = 34


def nt(a, b):
    return lax.dot_general(a, b, (((1,), (1,)), ((), ())), preferred_element_type=F32)


def nn(a, b):
    return lax.dot_general(a, b, (((1,), (0,)), ((), ())), preferred_element_type=F32)


def norm(x, gain):
    x = x.astype(F32)
    mean = jnp.mean(x, axis=-1, keepdims=True)
    cen = x - mean
    var = jnp.mean(cen * cen, axis=-1, keepdims=True)
    return (cen * lax.rsqrt(var + EPS) * gain).astype(BF)


def kernel(
    shard,
    fields,
    region,
    gain_a,
    gain_m,
    toks,
    out,
    gat,
    fx,
    reg,
    w_qkv,
    w_p,
    w_d,
    xb,
    q_s,
    k_s,
    v_s,
    bm,
    bt,
    mix,
    ox,
    ic,
    km_mask,
    tq_mask,
    to_mask,
    om_mask,
    ob,
    send,
    recv,
    loc,
    hsend,
    hrecv,
    osem,
):
    mem = lax.axis_index("mem")
    lat = lax.axis_index("lat")
    lon = lax.axis_index("lon")
    core = mem % 2
    y_lo = mem // 2
    y_hi = lon // 4
    x0 = lon % 4
    y0 = y_hi * 2 + y_lo
    pos = (x0, y0, lat)

    def dev(x, y, z, c):
        return ((y % 2) * 2 + c, z, (y // 2) * 4 + x)

    def moved(axis, dist, c=None):
        p = list(pos)
        p[axis] = (p[axis] + dist) % 4
        return dev(*p, core if c is None else c)

    sibling = dev(*pos, 1 - core)
    lat_b, lat_f = (lat + 3) % 4, (lat + 1) % 4
    lon_b, lon_f = (lon + 7) % 8, (lon + 1) % 8

    bar = pltpu.get_barrier_semaphore()
    peers = [moved(a, d) for a in range(3) for d in (1, 2, 3)] + [sibling]
    peers += [(mem, lat, lon_b), (mem, lat, lon_f), (mem, lat_b, lon_b), (mem, lat_f, lon_f)]
    for d in peers:
        pl.semaphore_signal(bar, inc=1, device_id=d, device_id_type=MESH)

    own = pltpu.make_async_copy(fields, fx.at[:, pl.ds(0, 24), pl.ds(0, 48)], loc.at[3])
    own.start()
    own_reg = pltpu.make_async_copy(region, reg.at[0, pl.ds(0, 24)], loc.at[4])
    own_reg.start()

    def chip(x, y, z, c):
        return (y % 2, c, z, y // 2, x)

    locals_ = []
    for p in range(3):
        cp = pltpu.make_async_copy(shard.at[p], gat.at[(p, *chip(*pos, core))], loc.at[p])
        cp.start()
        locals_.append(cp)

    pl.semaphore_wait(bar, len(peers))

    def remote(src, dst, s, r, d):
        cp = pltpu.make_async_remote_copy(
            src_ref=src, dst_ref=dst, send_sem=s, recv_sem=r, device_id=d, device_id_type=MESH
        )
        cp.start()
        return cp

    pend = []

    def blk(p, bval, cval, c):
        a, b, cc = p, (p + 1) % 3, (p + 2) % 3
        v = [None, None, None]
        v[b], v[cc] = bval, cval
        x, y, z = v
        full = pl.ds(0, 4)
        if y is None:
            yl, yh = pl.ds(0, 2), pl.ds(0, 2)
        else:
            yl, yh = y % 2, y // 2
        x = full if x is None else x
        z = full if z is None else z
        return gat.at[p, yl, c, z, yh, x]

    ph1 = {}
    for p in range(3):
        for i, d in enumerate((1, 3, 2)):
            here = gat.at[(p, *chip(*pos, core))]
            ph1[p, i] = remote(
                shard.at[p], here, send.at[p, S_P1 + i], recv.at[p, S_P1 + i], moved(p, d)
            )
            pend.append(ph1[p, i])

    halos = []
    fsl = (
        (fields.at[:, pl.ds(0, 3)], fx.at[:, pl.ds(24, 3), pl.ds(0, 48)], (mem, lat_b, lon)),
        (fields.at[:, :, pl.ds(0, 8)], fx.at[:, pl.ds(0, 24), pl.ds(48, 8)], (mem, lat, lon_b)),
        (
            fields.at[:, pl.ds(0, 3), pl.ds(0, 8)],
            fx.at[:, pl.ds(24, 3), pl.ds(48, 8)],
            (mem, lat_b, lon_b),
        ),
        (region, reg.at[0, pl.ds(24, 24)], (mem, lat_b, lon)),
        (region, reg.at[1, pl.ds(0, 24)], (mem, lat, lon_b)),
        (region, reg.at[1, pl.ds(24, 24)], (mem, lat_b, lon_b)),
    )
    for i, (s, t, d) in enumerate(fsl):
        halos.append(remote(s, t, hsend.at[i], hrecv.at[i], d))

    for cp in locals_:
        cp.wait()

    b0 = [pos[(p + 1) % 3] for p in range(3)]
    c0 = [pos[(p + 2) % 3] for p in range(3)]
    ph2, up, down, fwd, swap = {}, {}, {}, {}, {}
    dists = (0, 3, 1, 2)

    def to_core(p, slot, bval, cval):
        r = blk(p, bval, cval, core)
        swap[p, slot] = remote(r, r, send.at[p, S_CO + slot], recv.at[p, S_CO + slot], sibling)
        pend.append(swap[p, slot])

    def to_last(p, i):
        bval = (b0[p] + dists[i]) % 4
        r = blk(p, bval, c0[p], core)
        ax = (p + 2) % 3
        up[p, i] = remote(r, r, send.at[p, S_UP + i], recv.at[p, S_UP + i], moved(ax, 1))
        down[p, i] = remote(r, r, send.at[p, S_DN + i], recv.at[p, S_DN + i], moved(ax, 3))
        pend.extend((up[p, i], down[p, i]))
        to_core(p, i, bval, c0[p])

    for p in range(3):
        for i in range(3):
            ph1[p, i].wait_recv()
        r = blk(p, b0[p], c0[p], core)
        for i, d in enumerate((1, 3, 2)):
            ph2[p, i] = remote(
                r, r, send.at[p, S_P2 + i], recv.at[p, S_P2 + i], moved((p + 1) % 3, d)
            )
            pend.append(ph2[p, i])
        to_last(p, 0)
    for i in range(3):
        for p in range(3):
            ph2[p, i].wait_recv()
            to_last(p, i + 1)

    lane = lax.broadcasted_iota(jnp.int32, (WTOK, 128), 1)
    for h in range(4):
        km_mask[h] = jnp.where((lane >> 5) == h, 1.0, 0.0).astype(BF)
    tr = lax.broadcasted_iota(jnp.int32, (128, 256), 0)
    tl = lax.broadcasted_iota(jnp.int32, (128, 256), 1)
    tq_mask[...] = jnp.where((tr >> 4) == (tl >> 5), 1.0, 0.0).astype(BF)
    to_mask[...] = jnp.where((tr >> 4) == (tl >> 5), 1.0, 0.0)
    tr = lax.broadcasted_iota(jnp.int32, (512, 128), 0)
    tl = lax.broadcasted_iota(jnp.int32, (512, 128), 1)
    om_mask[...] = jnp.where((tr >> 7) == (tl >> 5), 1.0, 0.0)

    is_up = core == 0
    for i in range(4):
        for p in range(3):
            bval = (b0[p] + dists[i]) % 4
            ax = (p + 2) % 3
            up[p, i].wait_recv()
            down[p, i].wait_recv()
            cval = jnp.where(is_up, (c0[p] + 3) % 4, (c0[p] + 1) % 4)
            step = jnp.where(is_up, 1, 3)
            r = blk(p, bval, cval, core)
            fwd[p, i] = remote(
                r, r, send.at[p, S_FW + i], recv.at[p, S_FW + i], moved(ax, step)
            )
            pend.append(fwd[p, i])
            to_core(p, 4 + i, bval, (c0[p] + 3) % 4)
            to_core(p, 8 + i, bval, (c0[p] + 1) % 4)
    for i in range(4):
        for p in range(3):
            bval = (b0[p] + dists[i]) % 4
            fwd[p, i].wait_recv()
            to_core(p, 12 + i, bval, (c0[p] + 2) % 4)
    for p in range(3):
        for i in range(16):
            swap[p, i].wait_recv()
    own.wait()
    own_reg.wait()
    for h in halos:
        h.wait_recv()

    @pl.loop(0, 32)
    def _(g):
        at = (g // 16, (g // 8) % 2, (g // 2) % 4, g % 2)
        v = gat[(0, *at)]
        w_qkv[pl.ds(pl.multiple_of(g * 48, 16), 48), :] = jnp.concatenate(
            [v[i, 0:12] for i in range(4)], axis=0
        )
        w_p[pl.ds(pl.multiple_of(g * 16, 16), 16), :] = jnp.concatenate(
            [v[i, 12:16] for i in range(4)], axis=0
        )
        u = gat[(2, *at)]
        for k in range(4):
            w_d[pl.ds(pl.multiple_of(g * 16, 16), 16), 512 * k : 512 * k + 512] = jnp.concatenate(
                [u[i, 4 * k : 4 * k + 4] for i in range(4)], axis=0
            )

    @pl.loop(0, 4)
    def _(b):
        for w in range(4):
            pieces = [
                fx[l, 6 * b + SH + i, WLON * w + SL : WLON * w + SL + WLON, :]
                for l in range(2)
                for i in range(WLAT)
            ]
            xw = norm(jnp.concatenate(pieces, axis=0), gain_a[...])
            xb[WTOK * w : WTOK * w + WTOK, :] = xw
        rows = pl.ds(pl.multiple_of(b * 576, 16), 576)
        for n in range(2):
            cols = slice(256 * n, 256 * n + 256)
            q = nt(xb[...], w_qkv[256 * n : 256 * n + 256, :])
            q_s[rows, cols] = (q * QSCALE).astype(BF)
            k = nt(xb[...], w_qkv[512 + 256 * n : 512 + 256 * n + 256, :])
            k_s[rows, cols] = k.astype(BF)
            v = nt(xb[...], w_qkv[1024 + 256 * n : 1024 + 256 * n + 256, :])
            v_s[rows, cols] = v.astype(BF)
    @pl.loop(0, 4)
    def _(b):
        for w in range(4):
            win = b * 4 + w
            row = toks[0] + (6 * b + SH)
            col = toks[1] + (WLON * w + SL)
            l48 = lax.broadcasted_iota(jnp.int32, (WTOK, 48), 1)
            sel = jnp.where(l48 == row, 1.0, 0.0).astype(BF)
            near = nn(sel, reg[0].astype(F32).astype(BF))
            far = nn(sel, reg[1].astype(F32).astype(BF))
            ids = jnp.sum(
                jnp.where(l48 == col, near, 0.0) + jnp.where(l48 + 48 == col, far, 0.0),
                axis=1,
                keepdims=True,
            )
            glob = lat * 24 + row
            glob = jnp.where(glob >= NLAT_ALL, glob - NLAT_ALL, glob)
            code = ids * 2.0 + jnp.where(glob < SH, 1.0, 0.0)
            hot = jnp.where(code == lane.astype(F32), 1.0, 0.0).astype(BF)
            bm[win] = (nt(hot, hot[0:128]) - 1.0) * (-NEG)
            bt[win] = (nt(hot, jnp.concatenate([hot[128:144]] * 8, axis=0)) - 1.0) * (-NEG)

    def window(b, w):
        win = b * 4 + w
        at0 = pl.multiple_of(win * WTOK, 16)
        rows = pl.ds(at0, WTOK)

        def softmax(s):
            e = jnp.exp2(s - jnp.max(s, axis=-2, keepdims=True))
            return (e * (1.0 / jnp.sum(e, axis=-2, keepdims=True))).astype(BF)

        for s in range(4):
            at = 128 * s
            k4 = k_s[rows, at : at + 128]
            q4 = q_s[pl.ds(at0, 128), at : at + 128]
            sc = nt(jnp.concatenate([k4 * km_mask[h] for h in range(4)], axis=0), q4)
            p = softmax(sc.reshape(4, WTOK, 128) + bm[win])
            p = jnp.concatenate([p[h].T for h in range(4)], axis=0)
            o = nn(p, v_s[rows, at : at + 128]) * om_mask[...]
            o = o[0:128] + o[128:256] + o[256:384] + o[384:512]
            mix[pl.ds(pl.multiple_of(w * WTOK, 16), 128), at : at + 128] = o.astype(BF)
        for g in range(2):
            at = 256 * g
            qt = q_s[pl.ds(pl.multiple_of(at0 + 128, 16), 16), at : at + 256]
            qt = jnp.concatenate([qt] * 8, axis=0) * tq_mask[...]
            p = softmax(nt(k_s[rows, at : at + 256], qt) + bt[win]).T
            o = nn(p, v_s[rows, at : at + 256]) * to_mask[...]
            acc = o[0:16]
            for h in range(1, 8):
                acc = acc + o[16 * h : 16 * h + 16]
            mix[pl.ds(pl.multiple_of(w * WTOK + 128, 16), 16), at : at + 256] = acc.astype(BF)

    zeros = jnp.zeros((8, D), BF)

    @pl.loop(0, 4)
    def _(b):
        @pl.loop(0, 2)
        def _(w):
            window(b, 2 * w)
            window(b, 2 * w + 1)

        ao = nt(mix[...], w_p[...]).astype(BF)
        for l in range(2):
            for i in range(WLAT):
                at = 72 * l + 12 * i
                pieces = [ao[WTOK * w + at : WTOK * w + at + 12] for w in range(4)]
                ox[l, 6 * b + SH + i] = jnp.concatenate(
                    [zeros[0:6], *pieces, zeros[0:2]], axis=0
                )

    backs = []
    bsl = (
        (ox.at[:, pl.ds(3, 21), pl.ds(48, 8)], ic.at[:, pl.ds(3, 21)], (mem, lat, lon_f)),
        (ox.at[:, pl.ds(24, 3), pl.ds(0, 48)], ox.at[:, pl.ds(0, 3), pl.ds(0, 48)], (mem, lat_f, lon)),
        (ox.at[:, pl.ds(24, 3), pl.ds(48, 8)], ic.at[:, pl.ds(0, 3)], (mem, lat_f, lon_f)),
    )
    for i, (s, t, d) in enumerate(bsl):
        backs.append(remote(s, t, hsend.at[6 + i], hrecv.at[6 + i], d))
    for cp in backs:
        cp.wait_recv()

    first = lax.broadcasted_iota(jnp.int32, (12, 8, D), 1) < SL

    outs = []
    for t in range(4):
        l, r = t // 2, 12 * (t % 2)
        att = ox[l, r : r + 12, 0:48, :].astype(F32)
        head = jnp.where(first, ic[l, r : r + 12].astype(F32), att[:, 0:8])
        att = jnp.concatenate([head, att[:, 8:48]], axis=1)
        res = (fx[l, r : r + 12, 0:48, :].astype(F32) + att).astype(BF).reshape(576, D)
        xb[...] = norm(res, gain_m[...])
        acc = res.astype(F32)
        for k in range(4):
            pre = nt(xb[...], gat[1, k // 2, k % 2].reshape(512, D))
            hid = (0.5 * pre * (1.0 + lax.erf(pre * 0.7071067811865476))).astype(BF)
            acc = acc + nt(hid, w_d[:, 512 * k : 512 * k + 512])
        ob[t] = acc.astype(BF).reshape(12, 48, D)
        cp = pltpu.make_async_copy(ob.at[t], out.at[l, pl.ds(r, 12)], osem.at[t])
        cp.start()
        outs.append(cp)

    for cp in pend + halos + backs:
        cp.wait_send()
    for cp in outs:
        cp.wait()


def body(fields, region, gain_attn, w_qkv, w_proj, gain_mlp, w_up, w_down):
    down = w_down.T.reshape(4, 4, D).transpose(1, 0, 2).reshape(16, D)
    shard = jnp.stack([jnp.concatenate([w_qkv.T, w_proj.T], axis=0), w_up.T, down])
    tok = jnp.arange(WTOK, dtype=jnp.int32)
    toks = jnp.stack([(tok // WLON) % WLAT, tok % WLON]).reshape(2, WTOK, 1)
    vm = pl.BlockSpec(memory_space=pltpu.VMEM)
    hbm = pl.BlockSpec(memory_space=pl.ANY)
    dma = pltpu.SemaphoreType.DMA
    out = pl.pallas_call(
        kernel,
        out_shape=jax.ShapeDtypeStruct((2, 24, 48, D), BF),
        in_specs=[hbm, hbm, hbm, vm, vm, vm],
        out_specs=hbm,
        scratch_shapes=[
            pltpu.VMEM((3, 2, 2, 4, 2, 4, 16, D), BF),
            pltpu.VMEM((2, 27, 56, D), BF),
            pltpu.VMEM((2, 48, 48), jnp.int32),
            pltpu.VMEM((3 * D, D), BF),
            pltpu.VMEM((D, D), BF),
            pltpu.VMEM((D, FF), BF),
            pltpu.VMEM((576, D), BF),
            pltpu.VMEM((2304, D), BF),
            pltpu.VMEM((2304, D), BF),
            pltpu.VMEM((2304, D), BF),
            pltpu.VMEM((16, WTOK, 128), F32),
            pltpu.VMEM((16, WTOK, 128), F32),
            pltpu.VMEM((576, D), BF),
            pltpu.VMEM((2, 27, 56, D), BF),
            pltpu.VMEM((2, 24, 8, D), BF),
            pltpu.VMEM((4, WTOK, 128), BF),
            pltpu.VMEM((128, 256), BF),
            pltpu.VMEM((128, 256), F32),
            pltpu.VMEM((512, 128), F32),
            pltpu.VMEM((4, 12, 48, D), BF),
            dma((3, S_ALL)),
            dma((3, S_ALL)),
            dma((5,)),
            dma((9,)),
            dma((9,)),
            dma((4,)),
        ],
        compiler_params=pltpu.CompilerParams(
            collective_id=0, has_side_effects=True, vmem_limit_bytes=66 * 2**20 - 2**21
        ),
        name="block",
    )(shard, fields[0], region, gain_attn.reshape(1, D), gain_mlp.reshape(1, D), toks)
    return out[None]


def solution(mesh):
    in_specs = (
        P("mem", None, "lat", "lon", None),
        P("lat", "lon"),
        P(),
        P(None, ("mem", "lat", "lon")),
        P(None, ("mem", "lat", "lon")),
        P(),
        P(None, ("mem", "lat", "lon")),
        P(None, ("mem", "lat", "lon")),
    )
    out_specs = P("mem", None, "lat", "lon", None)
    return jax.shard_map(body, mesh=mesh, in_specs=in_specs, out_specs=out_specs, check_vma=False)
```

```python
import functools

import jax
import jax.numpy as jnp
from jax import lax
from jax.experimental import pallas as pl
from jax.experimental.pallas import tpu as pltpu
from jax.sharding import PartitionSpec as P

D = 512
FF = 2048
HDIM = 32
WLAT = 6
WLON = 12
WTOK = 144
SH = 3
SL = 6
NLAT_ALL = 96
QSCALE = 1.4426950408889634 / HDIM**0.5
NEG = -1e30
EPS = 1e-05
MESH = pl.DeviceIdType.MESH
BF = jnp.bfloat16
F32 = jnp.float32

UNITS = (
    (0, 0, (0, 2, 1)),
    (0, 1, (0, 1, 2)),
    (1, 0, (1, 2, 0)),
    (1, 1, (2, 1, 0)),
    (2, 0, (2, 0, 1)),
    (2, 1, (1, 0, 2)),
)
FIRST, LATER = (0, 1), (2, 3, 4, 5)


def nt(a, b):
    return lax.dot_general(a, b, (((1,), (1,)), ((), ())), preferred_element_type=F32)


def nn(a, b):
    return lax.dot_general(a, b, (((1,), (0,)), ((), ())), preferred_element_type=F32)


def norm(x, gain):
    x = x.astype(F32)
    mean = jnp.mean(x, axis=-1, keepdims=True)
    cen = x - mean
    var = jnp.mean(cen * cen, axis=-1, keepdims=True)
    return (cen * lax.rsqrt(var + EPS) * gain).astype(BF)


def kernel(
    w_qkv_in,
    w_p_in,
    w_u_in,
    w_d_in,
    fields,
    region,
    gain_a,
    gain_m,
    out,
    gat,
    fx,
    reg,
    w_qkv,
    w_p,
    w_d,
    xw,
    xb,
    q_s,
    k_s,
    v_s,
    bm,
    bt,
    mix,
    ox,
    ic,
    km_mask,
    tq_mask,
    to_mask,
    om_mask,
    ob,
    send,
    recv,
    loc,
    hsend,
    hrecv,
    bsend,
    brecv,
    osem,
):
    mem = lax.axis_index("mem")
    lat = lax.axis_index("lat")
    lon = lax.axis_index("lon")
    core = mem % 2
    y_lo = mem // 2
    y_hi = lon // 4
    x0 = lon % 4
    y0 = y_hi * 2 + y_lo
    pos = (x0, y0, lat)

    def dev(x, y, z, c):
        return ((y % 2) * 2 + c, z, (y // 2) * 4 + x)

    def moved(axis, dist, c=None):
        p = list(pos)
        p[axis] = (p[axis] + dist) % 4
        return dev(*p, core if c is None else c)

    sibling = dev(*pos, 1 - core)
    lat_b, lat_f = (lat + 3) % 4, (lat + 1) % 4
    lon_b, lon_f = (lon + 7) % 8, (lon + 1) % 8

    bar = pltpu.get_barrier_semaphore()
    peers = [moved(a, d) for a in range(3) for d in (1, 2, 3)] + [sibling]
    peers += [(mem, lat, lon_b), (mem, lat, lon_f), (mem, lat_b, lon_b), (mem, lat_f, lon_f)]
    for d in peers:
        pl.semaphore_signal(bar, inc=1, device_id=d, device_id_type=MESH)

    own = pltpu.make_async_copy(fields, fx.at[:, pl.ds(0, 24), pl.ds(0, 48)], loc.at[0])
    own.start()
    own_reg = pltpu.make_async_copy(region, reg.at[0, pl.ds(0, 24)], loc.at[1])
    own_reg.start()

    here = (y_lo, core, lat, y_hi, x0)
    gat[(0, *here)] = jnp.concatenate([w_qkv_in[...], w_p_in[...]], axis=0)
    gat[(1, *here)] = w_u_in[...]
    gat[(2, *here)] = jnp.concatenate(
        [w_d_in[:, 512 * k : 512 * k + 512] for k in range(4)], axis=0
    )

    def remote(src, dst, s, r, d):
        return pltpu.make_async_remote_copy(
            src_ref=src, dst_ref=dst, send_sem=s, recv_sem=r, device_id=d, device_id_type=MESH
        )

    def block(u, free, at=None):
        p, h, _ = UNITS[u]
        at = at or pos
        x = pl.ds(0, 4) if 0 in free else at[0]
        yl, yh = (pl.ds(0, 2), pl.ds(0, 2)) if 1 in free else (at[1] % 2, at[1] // 2)
        z = pl.ds(0, 4) if 2 in free else at[2]
        return gat.at[p, yl, core, z, yh, x, pl.ds(8 * h, 8)]

    steps = {}
    for u, (_, _, order) in enumerate(UNITS):
        for ph in range(3):
            r = block(u, order[:ph])
            for i, d in enumerate((1, 3, 2)):
                k = 3 * ph + i
                steps[u, ph, i] = remote(
                    r, r, send.at[u, k], recv.at[u, k], moved(order[ph], d)
                )
        for i, d in enumerate((0, 1, 3, 2)):
            at = list(pos)
            at[order[2]] = (at[order[2]] + 4 - d) % 4
            r = block(u, order[:2], at)
            steps[u, 3, i] = remote(r, r, send.at[u, 9 + i], recv.at[u, 9 + i], sibling)

    def start(units, ph, slots=(0, 1, 2)):
        for i in slots:
            for u in units:
                steps[u, ph, i].start()

    def arrived(units, ph, slots=(0, 1, 2)):
        for i in slots:
            for u in units:
                steps[u, ph, i].wait_recv()

    fsl = (
        (fields.at[:, :, pl.ds(0, 8)], fx.at[:, pl.ds(0, 24), pl.ds(48, 8)], (mem, lat, lon_b)),
        (fields.at[:, pl.ds(0, 3)], fx.at[:, pl.ds(24, 3), pl.ds(0, 48)], (mem, lat_b, lon)),
        (
            fields.at[:, pl.ds(0, 3), pl.ds(0, 8)],
            fx.at[:, pl.ds(24, 3), pl.ds(48, 8)],
            (mem, lat_b, lon_b),
        ),
        (region, reg.at[0, pl.ds(24, 24)], (mem, lat_b, lon)),
        (region, reg.at[1, pl.ds(0, 24)], (mem, lat, lon_b)),
        (region, reg.at[1, pl.ds(24, 24)], (mem, lat_b, lon_b)),
    )
    halos = [remote(s, t, hsend.at[i], hrecv.at[i], d) for i, (s, t, d) in enumerate(fsl)]

    def slab(b):
        rr = pl.ds(6 * b + SH, WLAT)
        return remote(
            ox.at[:, rr, pl.ds(48, 8)], ic.at[:, rr], bsend.at[b], brecv.at[b], (mem, lat, lon_f)
        )

    bsl = (
        (ox.at[:, pl.ds(24, 3), pl.ds(0, 48)], ox.at[:, pl.ds(0, 3), pl.ds(0, 48)], (mem, lat_f, lon)),
        (ox.at[:, pl.ds(24, 3), pl.ds(48, 8)], ic.at[:, pl.ds(0, 3)], (mem, lat_f, lon_f)),
    )
    backs = [
        remote(s, t, bsend.at[4 + i], brecv.at[4 + i], d) for i, (s, t, d) in enumerate(bsl)
    ]

    pl.semaphore_wait(bar, len(peers))
    start(FIRST, 0)
    for i in (3, 4, 5, 0):
        halos[i].start()
    start(LATER, 0)

    lane = lax.broadcasted_iota(jnp.int32, (WTOK, 128), 1)
    for h in range(4):
        km_mask[h] = jnp.where((lane >> 5) == h, 1.0, 0.0).astype(BF)
    tr = lax.broadcasted_iota(jnp.int32, (128, 256), 0)
    tl = lax.broadcasted_iota(jnp.int32, (128, 256), 1)
    tq_mask[...] = jnp.where((tr >> 4) == (tl >> 5), 1.0, 0.0).astype(BF)
    to_mask[...] = jnp.where((tr >> 4) == (tl >> 5), 1.0, 0.0)
    tr = lax.broadcasted_iota(jnp.int32, (512, 128), 0)
    tl = lax.broadcasted_iota(jnp.int32, (512, 128), 1)
    om_mask[...] = jnp.where((tr >> 7) == (tl >> 5), 1.0, 0.0)

    def cut(b, w):
        pieces = [
            fx[l, 6 * b + SH + i, WLON * w + SL : WLON * w + SL + WLON, :]
            for l in range(2)
            for i in range(WLAT)
        ]
        rows = pl.ds(pl.multiple_of((b * 4 + w) * WTOK, 16), WTOK)
        xw[rows, :] = norm(jnp.concatenate(pieces, axis=0), gain_a[...])

    arrived(FIRST, 0)
    start(FIRST, 1)
    own.wait()

    @pl.loop(0, 3)
    def _(b):
        for w in range(3):
            cut(b, w)

    arrived(FIRST, 1)
    start(FIRST, 2)
    start(FIRST, 3, (0,))
    for i in (1, 2):
        halos[i].start()
    arrived(LATER, 0)
    start(LATER, 1)

    own_reg.wait()
    for i in (3, 4, 5):
        halos[i].wait_recv()
    tok = lax.broadcasted_iota(jnp.int32, (WTOK, 1), 0)
    tok = jnp.where(tok >= 72, tok - 72, tok)
    tok_i = sum(jnp.where(tok >= 12 * k, 1, 0) for k in range(1, WLAT))
    tok_j = tok - 12 * tok_i

    @pl.loop(0, 4)
    def _(b):
        for w in range(4):
            win = b * 4 + w
            row = tok_i + (6 * b + SH)
            col = tok_j + (WLON * w + SL)
            l48 = lax.broadcasted_iota(jnp.int32, (WTOK, 48), 1)
            sel = jnp.where(l48 == row, 1.0, 0.0).astype(BF)
            near = nn(sel, reg[0].astype(F32).astype(BF))
            far = nn(sel, reg[1].astype(F32).astype(BF))
            ids = jnp.sum(
                jnp.where(l48 == col, near, 0.0) + jnp.where(l48 + 48 == col, far, 0.0),
                axis=1,
                keepdims=True,
            )
            glob = lat * 24 + row
            glob = jnp.where(glob >= NLAT_ALL, glob - NLAT_ALL, glob)
            code = ids * 2.0 + jnp.where(glob < SH, 1.0, 0.0)
            hot = jnp.where(code == lane.astype(F32), 1.0, 0.0).astype(BF)
            bm[win] = (nt(hot, hot[0:128]) - 1.0) * (-NEG)
            bt[win] = (nt(hot, jnp.concatenate([hot[128:144]] * 8, axis=0)) - 1.0) * (-NEG)

    halos[0].wait_recv()

    @pl.loop(0, 3)
    def _(b):
        cut(b, 3)

    for i in range(3):
        arrived(FIRST, 2, (i,))
        start(FIRST, 3, (i + 1,))
    arrived(FIRST, 3, (0, 1, 2, 3))

    @pl.loop(0, 32)
    def _(g):
        at = (g // 16, (g // 8) % 2, (g // 2) % 4, g % 2)
        v = gat[(0, *at)]
        w_qkv[pl.ds(pl.multiple_of(g * 48, 16), 48), :] = jnp.concatenate(
            [v[i, 0:12] for i in range(4)], axis=0
        )
        w_p[pl.ds(pl.multiple_of(g * 16, 16), 16), :] = jnp.concatenate(
            [v[i, 12:16] for i in range(4)], axis=0
        )

    @pl.loop(0, 4)
    def _(b):
        @pl.when(b == 1)
        def _():
            arrived(LATER, 1)
            start(LATER, 2)
            start(LATER, 3, (0,))

        @pl.when(b == 3)
        def _():
            halos[1].wait_recv()
            halos[2].wait_recv()
            for w in range(4):
                cut(3, w)

        rows = pl.ds(pl.multiple_of(b * 576, 16), 576)
        for n in range(2):
            cols = slice(256 * n, 256 * n + 256)
            q = nt(xw[rows, :], w_qkv[256 * n : 256 * n + 256, :])
            q_s[rows, cols] = (q * QSCALE).astype(BF)
            k = nt(xw[rows, :], w_qkv[512 + 256 * n : 512 + 256 * n + 256, :])
            k_s[rows, cols] = k.astype(BF)
            v = nt(xw[rows, :], w_qkv[1024 + 256 * n : 1024 + 256 * n + 256, :])
            v_s[rows, cols] = v.astype(BF)

    def window(b, w):
        win = b * 4 + w
        at0 = pl.multiple_of(win * WTOK, 16)
        rows = pl.ds(at0, WTOK)

        def softmax(s):
            e = jnp.exp2(s - jnp.max(s, axis=-2, keepdims=True))
            return (e * (1.0 / jnp.sum(e, axis=-2, keepdims=True))).astype(BF)

        for s in range(4):
            at = 128 * s
            k4 = k_s[rows, at : at + 128]
            q4 = q_s[pl.ds(at0, 128), at : at + 128]
            sc = nt(jnp.concatenate([k4 * km_mask[h] for h in range(4)], axis=0), q4)
            p = softmax(sc.reshape(4, WTOK, 128) + bm[win])
            p = jnp.concatenate([p[h].T for h in range(4)], axis=0)
            o = nn(p, v_s[rows, at : at + 128]) * om_mask[...]
            o = o[0:128] + o[128:256] + o[256:384] + o[384:512]
            mix[pl.ds(pl.multiple_of(w * WTOK, 16), 128), at : at + 128] = o.astype(BF)
        for g in range(2):
            at = 256 * g
            qt = q_s[pl.ds(pl.multiple_of(at0 + 128, 16), 16), at : at + 256]
            qt = jnp.concatenate([qt] * 8, axis=0) * tq_mask[...]
            p = softmax(nt(k_s[rows, at : at + 256], qt) + bt[win]).T
            o = nn(p, v_s[rows, at : at + 256]) * to_mask[...]
            acc = o[0:16]
            for h in range(1, 8):
                acc = acc + o[16 * h : 16 * h + 16]
            mix[pl.ds(pl.multiple_of(w * WTOK + 128, 16), 16), at : at + 256] = acc.astype(BF)

    zeros = jnp.zeros((8, D), BF)

    @pl.loop(0, 4)
    def _(turn):
        b = (turn + 3) % 4

        @pl.loop(0, 2)
        def _(w):
            window(b, 2 * w)
            window(b, 2 * w + 1)

        ao = nt(mix[...], w_p[...]).astype(BF)
        for l in range(2):
            for i in range(WLAT):
                at = 72 * l + 12 * i
                pieces = [ao[WTOK * w + at : WTOK * w + at + 12] for w in range(4)]
                ox[l, 6 * b + SH + i] = jnp.concatenate(
                    [zeros[0:6], *pieces, zeros[0:2]], axis=0
                )
        slab(b).start()

        @pl.when(turn == 0)
        def _():
            for cp in backs:
                cp.start()

        @pl.when(turn == 1)
        def _():
            arrived(LATER, 2)
            start(LATER, 3, (1, 2, 3))

    arrived(LATER, 3, (0, 1, 2, 3))

    @pl.loop(0, 32)
    def _(g):
        u = gat[(2, g // 16, (g // 8) % 2, (g // 2) % 4, g % 2)]
        for k in range(4):
            w_d[pl.ds(pl.multiple_of(g * 16, 16), 16), 512 * k : 512 * k + 512] = jnp.concatenate(
                [u[i, 4 * k : 4 * k + 4] for i in range(4)], axis=0
            )

    first = lax.broadcasted_iota(jnp.int32, (12, 8, D), 1) < SL

    outs = []
    for t in range(4):
        l, r = t % 2, 12 * (t // 2)
        if t == 0:
            for cp in (*backs, slab(0), slab(1)):
                cp.wait_recv()
        if t == 2:
            for cp in (slab(3), slab(2)):
                cp.wait_recv()
        att = ox[l, r : r + 12, 0:48, :].astype(F32)
        head = jnp.where(first, ic[l, r : r + 12].astype(F32), att[:, 0:8])
        att = jnp.concatenate([head, att[:, 8:48]], axis=1)
        res = (fx[l, r : r + 12, 0:48, :].astype(F32) + att).astype(BF).reshape(576, D)
        xb[...] = norm(res, gain_m[...])
        acc = res.astype(F32)
        for k in range(4):
            pre = nt(xb[...], gat[1, k // 2, k % 2].reshape(512, D))
            hid = (0.5 * pre * (1.0 + lax.erf(pre * 0.7071067811865476))).astype(BF)
            acc = acc + nt(hid, w_d[:, 512 * k : 512 * k + 512])
        ob[t] = acc.astype(BF).reshape(12, 48, D)
        cp = pltpu.make_async_copy(ob.at[t], out.at[l, pl.ds(r, 12)], osem.at[t])
        cp.start()
        outs.append(cp)

    for cp in (*steps.values(), *halos, *backs, *(slab(b) for b in range(4))):
        cp.wait_send()
    for cp in outs:
        cp.wait()


def body(fields, region, gain_attn, w_qkv, w_proj, gain_mlp, w_up, w_down):
    vm = pl.BlockSpec(memory_space=pltpu.VMEM)
    hbm = pl.BlockSpec(memory_space=pl.ANY)
    dma = pltpu.SemaphoreType.DMA
    out = pl.pallas_call(
        kernel,
        out_shape=jax.ShapeDtypeStruct((2, 24, 48, D), BF),
        in_specs=[vm, vm, vm, vm, hbm, hbm, vm, vm],
        out_specs=hbm,
        scratch_shapes=[
            pltpu.VMEM((3, 2, 2, 4, 2, 4, 16, D), BF),
            pltpu.VMEM((2, 27, 56, D), BF),
            pltpu.VMEM((2, 48, 48), jnp.int32),
            pltpu.VMEM((3 * D, D), BF),
            pltpu.VMEM((D, D), BF),
            pltpu.VMEM((D, FF), BF),
            pltpu.VMEM((2304, D), BF),
            pltpu.VMEM((576, D), BF),
            pltpu.VMEM((2304, D), BF),
            pltpu.VMEM((2304, D), BF),
            pltpu.VMEM((2304, D), BF),
            pltpu.VMEM((16, WTOK, 128), F32),
            pltpu.VMEM((16, WTOK, 128), F32),
            pltpu.VMEM((576, D), BF),
            pltpu.VMEM((2, 27, 56, D), BF),
            pltpu.VMEM((2, 27, 8, D), BF),
            pltpu.VMEM((4, WTOK, 128), BF),
            pltpu.VMEM((128, 256), BF),
            pltpu.VMEM((128, 256), F32),
            pltpu.VMEM((512, 128), F32),
            pltpu.VMEM((4, 12, 48, D), BF),
            dma((6, 13)),
            dma((6, 13)),
            dma((2,)),
            dma((6,)),
            dma((6,)),
            dma((6,)),
            dma((6,)),
            dma((4,)),
        ],
        compiler_params=pltpu.CompilerParams(
            collective_id=0, has_side_effects=True, vmem_limit_bytes=66 * 2**20 - 2**21
        ),
        name="block",
    )(
        w_qkv.T,
        w_proj.T,
        w_up.T,
        w_down.T,
        fields[0],
        region,
        gain_attn.reshape(1, D),
        gain_mlp.reshape(1, D),
    )
    return out[None]


def solution(mesh):
    in_specs = (
        P("mem", None, "lat", "lon", None),
        P("lat", "lon"),
        P(),
        P(None, ("mem", "lat", "lon")),
        P(None, ("mem", "lat", "lon")),
        P(),
        P(None, ("mem", "lat", "lon")),
        P(None, ("mem", "lat", "lon")),
    )
    out_specs = P("mem", None, "lat", "lon", None)
    return jax.shard_map(body, mesh=mesh, in_specs=in_specs, out_specs=out_specs, check_vma=False)
```

```python
import functools

import jax
import jax.numpy as jnp
from jax import lax
from jax.experimental import pallas as pl
from jax.experimental.pallas import tpu as pltpu
from jax.sharding import PartitionSpec as P

D = 512
FF = 2048
HDIM = 32
WLAT = 6
WLON = 12
WTOK = 144
SH = 3
SL = 6
NLAT_ALL = 96
QSCALE = 1.4426950408889634 / HDIM**0.5
NEG = -1e30
EPS = 1e-05
MESH = pl.DeviceIdType.MESH
BF = jnp.bfloat16
F32 = jnp.float32

UNITS = (
    (0, 0, (0, 2, 1)),
    (0, 1, (1, 2, 0)),
    (1, 0, (1, 2, 0)),
    (1, 1, (2, 1, 0)),
    (2, 0, (2, 0, 1)),
    (2, 1, (1, 0, 2)),
)
FIRST, LATER = (0, 1), (2, 3, 4, 5)


def nt(a, b):
    return lax.dot_general(a, b, (((1,), (1,)), ((), ())), preferred_element_type=F32)


def nn(a, b):
    return lax.dot_general(a, b, (((1,), (0,)), ((), ())), preferred_element_type=F32)


def norm(x, gain):
    x = x.astype(F32)
    mean = jnp.mean(x, axis=-1, keepdims=True)
    cen = x - mean
    var = jnp.mean(cen * cen, axis=-1, keepdims=True)
    return (cen * lax.rsqrt(var + EPS) * gain).astype(BF)


def kernel(
    w_qkv_in,
    w_p_in,
    w_u_in,
    w_d_in,
    fields,
    region,
    gain_a,
    gain_m,
    out,
    gat,
    fx,
    reg,
    w_qkv,
    w_p,
    w_d,
    xw,
    xb,
    q_s,
    k_s,
    v_s,
    bm,
    bt,
    mix,
    ox,
    ic,
    km_mask,
    tq_mask,
    to_mask,
    om_mask,
    ob,
    send,
    recv,
    loc,
    hsend,
    hrecv,
    bsend,
    brecv,
    osem,
):
    mem = lax.axis_index("mem")
    lat = lax.axis_index("lat")
    lon = lax.axis_index("lon")
    core = mem % 2
    y_lo = mem // 2
    y_hi = lon // 4
    x0 = lon % 4
    y0 = y_hi * 2 + y_lo
    pos = (x0, y0, lat)

    def dev(x, y, z, c):
        return ((y % 2) * 2 + c, z, (y // 2) * 4 + x)

    def moved(axis, dist, c=None):
        p = list(pos)
        p[axis] = (p[axis] + dist) % 4
        return dev(*p, core if c is None else c)

    sibling = dev(*pos, 1 - core)
    lat_b, lat_f = (lat + 3) % 4, (lat + 1) % 4
    lon_b, lon_f = (lon + 7) % 8, (lon + 1) % 8

    bar = pltpu.get_barrier_semaphore()
    peers = [moved(a, d) for a in range(3) for d in (1, 2, 3)] + [sibling]
    peers += [(mem, lat, lon_b), (mem, lat, lon_f), (mem, lat_b, lon_b), (mem, lat_f, lon_f)]
    for d in peers:
        pl.semaphore_signal(bar, inc=1, device_id=d, device_id_type=MESH)

    own = pltpu.make_async_copy(fields, fx.at[:, pl.ds(0, 24), pl.ds(0, 48)], loc.at[0])
    own.start()
    own_reg = pltpu.make_async_copy(region, reg.at[0, pl.ds(0, 24)], loc.at[1])
    own_reg.start()

    here = (y_lo, core, lat, y_hi, x0)
    gat[(0, *here)] = jnp.concatenate([w_qkv_in[...], w_p_in[...]], axis=0)
    gat[(1, *here)] = w_u_in[...]
    gat[(2, *here)] = jnp.concatenate(
        [w_d_in[:, 512 * k : 512 * k + 512] for k in range(4)], axis=0
    )

    def remote(src, dst, s, r, d):
        return pltpu.make_async_remote_copy(
            src_ref=src, dst_ref=dst, send_sem=s, recv_sem=r, device_id=d, device_id_type=MESH
        )

    def block(u, free, at=None):
        p, h, _ = UNITS[u]
        at = at or pos
        x = pl.ds(0, 4) if 0 in free else at[0]
        yl, yh = (pl.ds(0, 2), pl.ds(0, 2)) if 1 in free else (at[1] % 2, at[1] // 2)
        z = pl.ds(0, 4) if 2 in free else at[2]
        return gat.at[p, yl, core, z, yh, x, pl.ds(8 * h, 8)]

    steps = {}
    for u, (_, _, order) in enumerate(UNITS):
        for ph in range(3):
            r = block(u, order[:ph])
            for i, d in enumerate((1, 3, 2)):
                k = 3 * ph + i
                steps[u, ph, i] = remote(
                    r, r, send.at[u, k], recv.at[u, k], moved(order[ph], d)
                )
        for i, d in enumerate((0, 1, 3, 2)):
            at = list(pos)
            at[order[2]] = (at[order[2]] + 4 - d) % 4
            r = block(u, order[:2], at)
            steps[u, 3, i] = remote(r, r, send.at[u, 9 + i], recv.at[u, 9 + i], sibling)

    def start(units, ph, slots=(0, 1, 2)):
        for i in slots:
            for u in units:
                steps[u, ph, i].start()

    def arrived(units, ph, slots=(0, 1, 2)):
        for i in slots:
            for u in units:
                steps[u, ph, i].wait_recv()

    fsl = (
        (fields.at[:, :, pl.ds(0, 8)], fx.at[:, pl.ds(0, 24), pl.ds(48, 8)], (mem, lat, lon_b)),
        (fields.at[:, pl.ds(0, 3)], fx.at[:, pl.ds(24, 3), pl.ds(0, 48)], (mem, lat_b, lon)),
        (
            fields.at[:, pl.ds(0, 3), pl.ds(0, 8)],
            fx.at[:, pl.ds(24, 3), pl.ds(48, 8)],
            (mem, lat_b, lon_b),
        ),
        (region, reg.at[0, pl.ds(24, 24)], (mem, lat_b, lon)),
        (region, reg.at[1, pl.ds(0, 24)], (mem, lat, lon_b)),
        (region, reg.at[1, pl.ds(24, 24)], (mem, lat_b, lon_b)),
    )
    halos = [remote(s, t, hsend.at[i], hrecv.at[i], d) for i, (s, t, d) in enumerate(fsl)]

    def slab(b):
        rr = pl.ds(6 * b + SH, WLAT)
        return remote(
            ox.at[:, rr, pl.ds(48, 8)], ic.at[:, rr], bsend.at[b], brecv.at[b], (mem, lat, lon_f)
        )

    bsl = (
        (ox.at[:, pl.ds(24, 3), pl.ds(0, 48)], ox.at[:, pl.ds(0, 3), pl.ds(0, 48)], (mem, lat_f, lon)),
        (ox.at[:, pl.ds(24, 3), pl.ds(48, 8)], ic.at[:, pl.ds(0, 3)], (mem, lat_f, lon_f)),
    )
    backs = [
        remote(s, t, bsend.at[4 + i], brecv.at[4 + i], d) for i, (s, t, d) in enumerate(bsl)
    ]

    pl.semaphore_wait(bar, len(peers))
    start(FIRST, 0)
    for i in (3, 4, 5, 0):
        halos[i].start()
    start(LATER, 0)

    lane = lax.broadcasted_iota(jnp.int32, (WTOK, 128), 1)
    for h in range(4):
        km_mask[h] = jnp.where((lane >> 5) == h, 1.0, 0.0).astype(BF)
    tr = lax.broadcasted_iota(jnp.int32, (128, 256), 0)
    tl = lax.broadcasted_iota(jnp.int32, (128, 256), 1)
    tq_mask[...] = jnp.where((tr >> 4) == (tl >> 5), 1.0, 0.0).astype(BF)
    to_mask[...] = jnp.where((tr >> 4) == (tl >> 5), 1.0, 0.0)
    tr = lax.broadcasted_iota(jnp.int32, (512, 128), 0)
    tl = lax.broadcasted_iota(jnp.int32, (512, 128), 1)
    om_mask[...] = jnp.where((tr >> 7) == (tl >> 5), 1.0, 0.0)

    def cut(b, w):
        pieces = [
            fx[l, 6 * b + SH + i, WLON * w + SL : WLON * w + SL + WLON, :]
            for l in range(2)
            for i in range(WLAT)
        ]
        rows = pl.ds(pl.multiple_of((b * 4 + w) * WTOK, 16), WTOK)
        xw[rows, :] = norm(jnp.concatenate(pieces, axis=0), gain_a[...])

    arrived(FIRST, 0)
    start(FIRST, 1)
    own.wait()

    @pl.loop(0, 3)
    def _(b):
        for w in range(3):
            cut(b, w)

    arrived(FIRST, 1)
    start(FIRST, 2)
    start(FIRST, 3, (0,))
    for i in (1, 2):
        halos[i].start()
    arrived(LATER, 0)
    start(LATER, 1)

    own_reg.wait()
    for i in (3, 4, 5):
        halos[i].wait_recv()
    tok = lax.broadcasted_iota(jnp.int32, (WTOK, 1), 0)
    tok = jnp.where(tok >= 72, tok - 72, tok)
    tok_i = sum(jnp.where(tok >= 12 * k, 1, 0) for k in range(1, WLAT))
    tok_j = tok - 12 * tok_i

    @pl.loop(0, 4)
    def _(b):
        for w in range(4):
            win = b * 4 + w
            row = tok_i + (6 * b + SH)
            col = tok_j + (WLON * w + SL)
            l48 = lax.broadcasted_iota(jnp.int32, (WTOK, 48), 1)
            sel = jnp.where(l48 == row, 1.0, 0.0).astype(BF)
            near = nn(sel, reg[0].astype(F32).astype(BF))
            far = nn(sel, reg[1].astype(F32).astype(BF))
            ids = jnp.sum(
                jnp.where(l48 == col, near, 0.0) + jnp.where(l48 + 48 == col, far, 0.0),
                axis=1,
                keepdims=True,
            )
            glob = lat * 24 + row
            glob = jnp.where(glob >= NLAT_ALL, glob - NLAT_ALL, glob)
            code = ids * 2.0 + jnp.where(glob < SH, 1.0, 0.0)
            hot = jnp.where(code == lane.astype(F32), 1.0, 0.0).astype(BF)
            bm[win] = (nt(hot, hot[0:128]) - 1.0) * (-NEG)
            bt[win] = (nt(hot, jnp.concatenate([hot[128:144]] * 8, axis=0)) - 1.0) * (-NEG)

    halos[0].wait_recv()

    @pl.loop(0, 3)
    def _(b):
        cut(b, 3)

    for i in range(3):
        arrived(FIRST, 2, (i,))
        start(FIRST, 3, (i + 1,))
    arrived(FIRST, 3, (0, 1, 2, 3))

    @pl.loop(0, 32)
    def _(g):
        at = (g // 16, (g // 8) % 2, (g // 2) % 4, g % 2)
        v = gat[(0, *at)]
        w_qkv[pl.ds(pl.multiple_of(g * 48, 16), 48), :] = jnp.concatenate(
            [v[i, 0:12] for i in range(4)], axis=0
        )
        w_p[pl.ds(pl.multiple_of(g * 16, 16), 16), :] = jnp.concatenate(
            [v[i, 12:16] for i in range(4)], axis=0
        )

    @pl.loop(0, 4)
    def _(b):
        @pl.when(b == 1)
        def _():
            arrived(LATER, 1)
            start(LATER, 2)
            start(LATER, 3, (0,))

        @pl.when(b == 3)
        def _():
            halos[1].wait_recv()
            halos[2].wait_recv()
            for w in range(4):
                cut(3, w)

        rows = pl.ds(pl.multiple_of(b * 576, 16), 576)
        for n in range(2):
            cols = slice(256 * n, 256 * n + 256)
            q = nt(xw[rows, :], w_qkv[256 * n : 256 * n + 256, :])
            q_s[rows, cols] = (q * QSCALE).astype(BF)
            k = nt(xw[rows, :], w_qkv[512 + 256 * n : 512 + 256 * n + 256, :])
            k_s[rows, cols] = k.astype(BF)
            v = nt(xw[rows, :], w_qkv[1024 + 256 * n : 1024 + 256 * n + 256, :])
            v_s[rows, cols] = v.astype(BF)

    def window(b, w):
        win = b * 4 + w
        at0 = pl.multiple_of(win * WTOK, 16)
        rows = pl.ds(at0, WTOK)

        def softmax(s):
            e = jnp.exp2(s - jnp.max(s, axis=-2, keepdims=True))
            return (e * (1.0 / jnp.sum(e, axis=-2, keepdims=True))).astype(BF)

        for s in range(4):
            at = 128 * s
            k4 = k_s[rows, at : at + 128]
            q4 = q_s[pl.ds(at0, 128), at : at + 128]
            sc = nt(jnp.concatenate([k4 * km_mask[h] for h in range(4)], axis=0), q4)
            p = softmax(sc.reshape(4, WTOK, 128) + bm[win])
            p = jnp.concatenate([p[h].T for h in range(4)], axis=0)
            o = nn(p, v_s[rows, at : at + 128]) * om_mask[...]
            o = o[0:128] + o[128:256] + o[256:384] + o[384:512]
            mix[pl.ds(pl.multiple_of(w * WTOK, 16), 128), at : at + 128] = o.astype(BF)
        for g in range(2):
            at = 256 * g
            qt = q_s[pl.ds(pl.multiple_of(at0 + 128, 16), 16), at : at + 256]
            qt = jnp.concatenate([qt] * 8, axis=0) * tq_mask[...]
            p = softmax(nt(k_s[rows, at : at + 256], qt) + bt[win]).T
            o = nn(p, v_s[rows, at : at + 256]) * to_mask[...]
            acc = o[0:16]
            for h in range(1, 8):
                acc = acc + o[16 * h : 16 * h + 16]
            mix[pl.ds(pl.multiple_of(w * WTOK + 128, 16), 16), at : at + 256] = acc.astype(BF)

    zeros = jnp.zeros((8, D), BF)

    @pl.loop(0, 4)
    def _(turn):
        b = (turn + 3) % 4

        @pl.loop(0, 2)
        def _(w):
            window(b, 2 * w)
            window(b, 2 * w + 1)

        ao = nt(mix[...], w_p[...]).astype(BF)
        for l in range(2):
            for i in range(WLAT):
                at = 72 * l + 12 * i
                pieces = [ao[WTOK * w + at : WTOK * w + at + 12] for w in range(4)]
                ox[l, 6 * b + SH + i] = jnp.concatenate(
                    [zeros[0:6], *pieces, zeros[0:2]], axis=0
                )
        slab(b).start()

        @pl.when(turn == 0)
        def _():
            for cp in backs:
                cp.start()

        @pl.when(turn == 1)
        def _():
            arrived(LATER, 2)
            start(LATER, 3, (1, 2, 3))

    arrived(LATER, 3, (0, 1, 2, 3))

    @pl.loop(0, 32)
    def _(g):
        u = gat[(2, g // 16, (g // 8) % 2, (g // 2) % 4, g % 2)]
        for k in range(4):
            w_d[pl.ds(pl.multiple_of(g * 16, 16), 16), 512 * k : 512 * k + 512] = jnp.concatenate(
                [u[i, 4 * k : 4 * k + 4] for i in range(4)], axis=0
            )

    first = lax.broadcasted_iota(jnp.int32, (12, 8, D), 1) < SL

    outs = []
    for t in range(4):
        l, r = t % 2, 12 * (t // 2)
        if t == 0:
            for cp in (*backs, slab(0), slab(1)):
                cp.wait_recv()
        if t == 2:
            for cp in (slab(3), slab(2)):
                cp.wait_recv()
        att = ox[l, r : r + 12, 0:48, :].astype(F32)
        head = jnp.where(first, ic[l, r : r + 12].astype(F32), att[:, 0:8])
        att = jnp.concatenate([head, att[:, 8:48]], axis=1)
        res = (fx[l, r : r + 12, 0:48, :].astype(F32) + att).astype(BF).reshape(576, D)
        xb[...] = norm(res, gain_m[...])
        acc = res.astype(F32)
        for k in range(4):
            pre = nt(xb[...], gat[1, k // 2, k % 2].reshape(512, D))
            hid = (0.5 * pre * (1.0 + lax.erf(pre * 0.7071067811865476))).astype(BF)
            acc = acc + nt(hid, w_d[:, 512 * k : 512 * k + 512])
        ob[t] = acc.astype(BF).reshape(12, 48, D)
        cp = pltpu.make_async_copy(ob.at[t], out.at[l, pl.ds(r, 12)], osem.at[t])
        cp.start()
        outs.append(cp)

    for cp in (*steps.values(), *halos, *backs, *(slab(b) for b in range(4))):
        cp.wait_send()
    for cp in outs:
        cp.wait()


def body(fields, region, gain_attn, w_qkv, w_proj, gain_mlp, w_up, w_down):
    vm = pl.BlockSpec(memory_space=pltpu.VMEM)
    hbm = pl.BlockSpec(memory_space=pl.ANY)
    dma = pltpu.SemaphoreType.DMA
    out = pl.pallas_call(
        kernel,
        out_shape=jax.ShapeDtypeStruct((2, 24, 48, D), BF),
        in_specs=[vm, vm, vm, vm, hbm, hbm, vm, vm],
        out_specs=hbm,
        scratch_shapes=[
            pltpu.VMEM((3, 2, 2, 4, 2, 4, 16, D), BF),
            pltpu.VMEM((2, 27, 56, D), BF),
            pltpu.VMEM((2, 48, 48), jnp.int32),
            pltpu.VMEM((3 * D, D), BF),
            pltpu.VMEM((D, D), BF),
            pltpu.VMEM((D, FF), BF),
            pltpu.VMEM((2304, D), BF),
            pltpu.VMEM((576, D), BF),
            pltpu.VMEM((2304, D), BF),
            pltpu.VMEM((2304, D), BF),
            pltpu.VMEM((2304, D), BF),
            pltpu.VMEM((16, WTOK, 128), F32),
            pltpu.VMEM((16, WTOK, 128), F32),
            pltpu.VMEM((576, D), BF),
            pltpu.VMEM((2, 27, 56, D), BF),
            pltpu.VMEM((2, 27, 8, D), BF),
            pltpu.VMEM((4, WTOK, 128), BF),
            pltpu.VMEM((128, 256), BF),
            pltpu.VMEM((128, 256), F32),
            pltpu.VMEM((512, 128), F32),
            pltpu.VMEM((4, 12, 48, D), BF),
            dma((6, 13)),
            dma((6, 13)),
            dma((2,)),
            dma((6,)),
            dma((6,)),
            dma((6,)),
            dma((6,)),
            dma((4,)),
        ],
        compiler_params=pltpu.CompilerParams(
            collective_id=0, has_side_effects=True, vmem_limit_bytes=66 * 2**20 - 2**21
        ),
        name="block",
    )(
        w_qkv.T,
        w_proj.T,
        w_up.T,
        w_down.T,
        fields[0],
        region,
        gain_attn.reshape(1, D),
        gain_mlp.reshape(1, D),
    )
    return out[None]


def solution(mesh):
    in_specs = (
        P("mem", None, "lat", "lon", None),
        P("lat", "lon"),
        P(),
        P(None, ("mem", "lat", "lon")),
        P(None, ("mem", "lat", "lon")),
        P(),
        P(None, ("mem", "lat", "lon")),
        P(None, ("mem", "lat", "lon")),
    )
    out_specs = P("mem", None, "lat", "lon", None)
    return jax.shard_map(body, mesh=mesh, in_specs=in_specs, out_specs=out_specs, check_vma=False)
```

```python
import functools

import jax
import jax.numpy as jnp
from jax import lax
from jax.experimental import pallas as pl
from jax.experimental.pallas import tpu as pltpu
from jax.sharding import PartitionSpec as P

D = 512
FF = 2048
HDIM = 32
WLAT = 6
WLON = 12
WTOK = 144
SH = 3
SL = 6
NLAT_ALL = 96
QSCALE = 1.4426950408889634 / HDIM**0.5
NEG = -1e30
EPS = 1e-05
MESH = pl.DeviceIdType.MESH
BF = jnp.bfloat16
F32 = jnp.float32

UNITS = (
    (0, 0, (0, 2, 1)),
    (0, 1, (1, 2, 0)),
    (1, 0, (1, 2, 0)),
    (1, 1, (2, 1, 0)),
    (2, 0, (2, 0, 1)),
    (2, 1, (1, 0, 2)),
)
FIRST, LATER = (0, 1), (2, 3, 4, 5)


def nt(a, b):
    return lax.dot_general(a, b, (((1,), (1,)), ((), ())), preferred_element_type=F32)


def nn(a, b):
    return lax.dot_general(a, b, (((1,), (0,)), ((), ())), preferred_element_type=F32)


def norm(x, gain):
    x = x.astype(F32)
    mean = jnp.mean(x, axis=-1, keepdims=True)
    cen = x - mean
    var = jnp.mean(cen * cen, axis=-1, keepdims=True)
    return (cen * lax.rsqrt(var + EPS) * gain).astype(BF)


def kernel(
    w_qkv_in,
    w_p_in,
    w_u_in,
    w_d_in,
    fields,
    region,
    gain_a,
    gain_m,
    out,
    gat,
    fx,
    reg,
    w_qkv,
    w_p,
    w_d,
    xw,
    xb,
    q_s,
    k_s,
    v_s,
    bm,
    bt,
    mix,
    ox,
    ic,
    km_mask,
    tq_mask,
    to_mask,
    om_mask,
    ob,
    send,
    recv,
    loc,
    hsend,
    hrecv,
    bsend,
    brecv,
    osem,
):
    mem = lax.axis_index("mem")
    lat = lax.axis_index("lat")
    lon = lax.axis_index("lon")
    core = mem % 2
    y_lo = mem // 2
    y_hi = lon // 4
    x0 = lon % 4
    y0 = y_hi * 2 + y_lo
    pos = (x0, y0, lat)

    def dev(x, y, z, c):
        return ((y % 2) * 2 + c, z, (y // 2) * 4 + x)

    def moved(axis, dist, c=None):
        p = list(pos)
        p[axis] = (p[axis] + dist) % 4
        return dev(*p, core if c is None else c)

    sibling = dev(*pos, 1 - core)
    lat_b, lat_f = (lat + 3) % 4, (lat + 1) % 4
    lon_b, lon_f = (lon + 7) % 8, (lon + 1) % 8

    bar = pltpu.get_barrier_semaphore()
    peers = [moved(a, d) for a in range(3) for d in (1, 2, 3)] + [sibling]
    peers += [(mem, lat, lon_b), (mem, lat, lon_f), (mem, lat_b, lon_b), (mem, lat_f, lon_f)]
    for d in peers:
        pl.semaphore_signal(bar, inc=1, device_id=d, device_id_type=MESH)

    own = pltpu.make_async_copy(fields, fx.at[:, pl.ds(0, 24), pl.ds(0, 48)], loc.at[0])
    own.start()
    own_reg = pltpu.make_async_copy(region, reg.at[0, pl.ds(0, 24)], loc.at[1])
    own_reg.start()

    here = (y_lo, core, lat, y_hi, x0)
    gat[(0, *here)] = jnp.concatenate([w_qkv_in[...], w_p_in[...]], axis=0)
    gat[(1, *here)] = w_u_in[...]
    gat[(2, *here)] = jnp.concatenate(
        [w_d_in[:, 512 * k : 512 * k + 512] for k in range(4)], axis=0
    )

    def remote(src, dst, s, r, d):
        return pltpu.make_async_remote_copy(
            src_ref=src, dst_ref=dst, send_sem=s, recv_sem=r, device_id=d, device_id_type=MESH
        )

    def block(u, free, at=None):
        p, h, _ = UNITS[u]
        at = at or pos
        x = pl.ds(0, 4) if 0 in free else at[0]
        yl, yh = (pl.ds(0, 2), pl.ds(0, 2)) if 1 in free else (at[1] % 2, at[1] // 2)
        z = pl.ds(0, 4) if 2 in free else at[2]
        return gat.at[p, yl, core, z, yh, x, pl.ds(8 * h, 8)]

    steps = {}
    for u, (_, _, order) in enumerate(UNITS):
        for ph in range(3):
            r = block(u, order[:ph])
            for i, d in enumerate((1, 3, 2)):
                k = 3 * ph + i
                steps[u, ph, i] = remote(
                    r, r, send.at[u, k], recv.at[u, k], moved(order[ph], d)
                )
        for i, d in enumerate((0, 1, 3, 2)):
            at = list(pos)
            at[order[2]] = (at[order[2]] + 4 - d) % 4
            r = block(u, order[:2], at)
            steps[u, 3, i] = remote(r, r, send.at[u, 9 + i], recv.at[u, 9 + i], sibling)

    def start(units, ph, slots=(0, 1, 2)):
        for i in slots:
            for u in units:
                steps[u, ph, i].start()

    def arrived(units, ph, slots=(0, 1, 2)):
        for i in slots:
            for u in units:
                steps[u, ph, i].wait_recv()

    fsl = (
        (fields.at[:, :, pl.ds(0, 8)], fx.at[:, pl.ds(0, 24), pl.ds(48, 8)], (mem, lat, lon_b)),
        (fields.at[:, pl.ds(0, 3)], fx.at[:, pl.ds(24, 3), pl.ds(0, 48)], (mem, lat_b, lon)),
        (
            fields.at[:, pl.ds(0, 3), pl.ds(0, 8)],
            fx.at[:, pl.ds(24, 3), pl.ds(48, 8)],
            (mem, lat_b, lon_b),
        ),
        (region, reg.at[0, pl.ds(24, 24)], (mem, lat_b, lon)),
        (region, reg.at[1, pl.ds(0, 24)], (mem, lat, lon_b)),
        (region, reg.at[1, pl.ds(24, 24)], (mem, lat_b, lon_b)),
    )
    halos = [remote(s, t, hsend.at[i], hrecv.at[i], d) for i, (s, t, d) in enumerate(fsl)]

    def slab(b):
        rr = pl.ds(6 * b + SH, WLAT)
        return remote(
            ox.at[:, rr, pl.ds(48, 8)], ic.at[:, rr], bsend.at[b], brecv.at[b], (mem, lat, lon_f)
        )

    bsl = (
        (ox.at[:, pl.ds(24, 3), pl.ds(0, 48)], ox.at[:, pl.ds(0, 3), pl.ds(0, 48)], (mem, lat_f, lon)),
        (ox.at[:, pl.ds(24, 3), pl.ds(48, 8)], ic.at[:, pl.ds(0, 3)], (mem, lat_f, lon_f)),
    )
    backs = [
        remote(s, t, bsend.at[4 + i], brecv.at[4 + i], d) for i, (s, t, d) in enumerate(bsl)
    ]

    pl.semaphore_wait(bar, len(peers))
    start(FIRST, 0)
    for i in (3, 4, 5, 0):
        halos[i].start()
    start(LATER, 0)

    lane = lax.broadcasted_iota(jnp.int32, (WTOK, 128), 1)
    for h in range(4):
        km_mask[h] = jnp.where((lane >> 5) == h, 1.0, 0.0).astype(BF)
    tr = lax.broadcasted_iota(jnp.int32, (128, 256), 0)
    tl = lax.broadcasted_iota(jnp.int32, (128, 256), 1)
    tq_mask[...] = jnp.where((tr >> 4) == (tl >> 5), 1.0, 0.0).astype(BF)
    to_mask[...] = jnp.where((tr >> 4) == (tl >> 5), 1.0, 0.0)
    tr = lax.broadcasted_iota(jnp.int32, (512, 128), 0)
    tl = lax.broadcasted_iota(jnp.int32, (512, 128), 1)
    om_mask[...] = jnp.where((tr >> 7) == (tl >> 5), 1.0, 0.0)

    def cut(b, w):
        pieces = [
            fx[l, 6 * b + SH + i, WLON * w + SL : WLON * w + SL + WLON, :]
            for l in range(2)
            for i in range(WLAT)
        ]
        rows = pl.ds(pl.multiple_of((b * 4 + w) * WTOK, 16), WTOK)
        xw[rows, :] = norm(jnp.concatenate(pieces, axis=0), gain_a[...])

    arrived(FIRST, 0)
    start(FIRST, 1)
    own.wait()

    @pl.loop(0, 3)
    def _(b):
        for w in range(3):
            cut(b, w)

    arrived(FIRST, 1)
    start(FIRST, 2)
    start(FIRST, 3, (0,))
    for i in (1, 2):
        halos[i].start()
    arrived(LATER, 0)
    start(LATER, 1)

    own_reg.wait()
    for i in (3, 4, 5):
        halos[i].wait_recv()
    tok = lax.broadcasted_iota(jnp.int32, (WTOK, 1), 0)
    tok = jnp.where(tok >= 72, tok - 72, tok)
    tok_i = sum(jnp.where(tok >= 12 * k, 1, 0) for k in range(1, WLAT))
    tok_j = tok - 12 * tok_i

    @pl.loop(0, 4)
    def _(b):
        for w in range(4):
            win = b * 4 + w
            row = tok_i + (6 * b + SH)
            col = tok_j + (WLON * w + SL)
            l48 = lax.broadcasted_iota(jnp.int32, (WTOK, 48), 1)
            sel = jnp.where(l48 == row, 1.0, 0.0).astype(BF)
            near = nn(sel, reg[0].astype(F32).astype(BF))
            far = nn(sel, reg[1].astype(F32).astype(BF))
            ids = jnp.sum(
                jnp.where(l48 == col, near, 0.0) + jnp.where(l48 + 48 == col, far, 0.0),
                axis=1,
                keepdims=True,
            )
            glob = lat * 24 + row
            glob = jnp.where(glob >= NLAT_ALL, glob - NLAT_ALL, glob)
            code = ids * 2.0 + jnp.where(glob < SH, 1.0, 0.0)
            hot = jnp.where(code == lane.astype(F32), 1.0, 0.0).astype(BF)
            bm[win] = (nt(hot, hot[0:128]) - 1.0) * (-NEG)
            bt[win] = (nt(hot, jnp.concatenate([hot[128:144]] * 8, axis=0)) - 1.0) * (-NEG)

    halos[0].wait_recv()

    @pl.loop(0, 3)
    def _(b):
        cut(b, 3)

    for i in range(3):
        arrived(FIRST, 2, (i,))
        start(FIRST, 3, (i + 1,))
    arrived(FIRST, 3, (0, 1, 2, 3))

    @pl.loop(0, 32)
    def _(g):
        at = (g // 16, (g // 8) % 2, (g // 2) % 4, g % 2)
        v = gat[(0, *at)]
        w_qkv[pl.ds(pl.multiple_of(g * 48, 16), 48), :] = jnp.concatenate(
            [v[i, 0:12] for i in range(4)], axis=0
        )
        w_p[pl.ds(pl.multiple_of(g * 16, 16), 16), :] = jnp.concatenate(
            [v[i, 12:16] for i in range(4)], axis=0
        )

    @pl.loop(0, 4)
    def _(b):
        @pl.when(b == 1)
        def _():
            arrived(LATER, 1)
            start(LATER, 2)
            start(LATER, 3, (0,))

        @pl.when(b == 3)
        def _():
            halos[1].wait_recv()
            halos[2].wait_recv()
            for w in range(4):
                cut(3, w)

        rows = pl.ds(pl.multiple_of(b * 576, 16), 576)
        for n in range(2):
            cols = slice(256 * n, 256 * n + 256)
            q = nt(xw[rows, :], w_qkv[256 * n : 256 * n + 256, :])
            q_s[rows, cols] = (q * QSCALE).astype(BF)
            k = nt(xw[rows, :], w_qkv[512 + 256 * n : 512 + 256 * n + 256, :])
            k_s[rows, cols] = k.astype(BF)
            v = nt(xw[rows, :], w_qkv[1024 + 256 * n : 1024 + 256 * n + 256, :])
            v_s[rows, cols] = v.astype(BF)

    def window(b, w):
        win = b * 4 + w
        at0 = pl.multiple_of(win * WTOK, 16)
        rows = pl.ds(at0, WTOK)

        def softmax(s):
            e = jnp.exp2(s - jnp.max(s, axis=-2, keepdims=True))
            return (e * (1.0 / jnp.sum(e, axis=-2, keepdims=True))).astype(BF)

        for s in range(4):
            at = 128 * s
            k4 = k_s[rows, at : at + 128]
            q4 = q_s[pl.ds(at0, 128), at : at + 128]
            sc = nt(jnp.concatenate([k4 * km_mask[h] for h in range(4)], axis=0), q4)
            p = softmax(sc.reshape(4, WTOK, 128) + bm[win])
            p = jnp.concatenate([p[h].T for h in range(4)], axis=0)
            o = nn(p, v_s[rows, at : at + 128]) * om_mask[...]
            o = o[0:128] + o[128:256] + o[256:384] + o[384:512]
            mix[pl.ds(pl.multiple_of(w * WTOK, 16), 128), at : at + 128] = o.astype(BF)
        for g in range(2):
            at = 256 * g
            qt = q_s[pl.ds(pl.multiple_of(at0 + 128, 16), 16), at : at + 256]
            qt = jnp.concatenate([qt] * 8, axis=0) * tq_mask[...]
            p = softmax(nt(k_s[rows, at : at + 256], qt) + bt[win]).T
            o = nn(p, v_s[rows, at : at + 256]) * to_mask[...]
            acc = o[0:16]
            for h in range(1, 8):
                acc = acc + o[16 * h : 16 * h + 16]
            mix[pl.ds(pl.multiple_of(w * WTOK + 128, 16), 16), at : at + 256] = acc.astype(BF)

    zeros = jnp.zeros((8, D), BF)

    @pl.loop(0, 4)
    def _(turn):
        b = (turn + 3) % 4

        @pl.loop(0, 2)
        def _(w):
            window(b, 2 * w)
            window(b, 2 * w + 1)

        ao = nt(mix[...], w_p[...]).astype(BF)
        for l in range(2):
            for i in range(WLAT):
                at = 72 * l + 12 * i
                pieces = [ao[WTOK * w + at : WTOK * w + at + 12] for w in range(4)]
                ox[l, 6 * b + SH + i] = jnp.concatenate(
                    [zeros[0:6], *pieces, zeros[0:2]], axis=0
                )
        slab(b).start()

        @pl.when(turn == 0)
        def _():
            for cp in backs:
                cp.start()

        @pl.when(turn == 1)
        def _():
            arrived(LATER, 2)
            start(LATER, 3, (1, 2, 3))

    arrived(LATER, 3, (0, 1, 2, 3))

    @pl.loop(0, 32)
    def _(g):
        u = gat[(2, g // 16, (g // 8) % 2, (g // 2) % 4, g % 2)]
        for k in range(4):
            w_d[pl.ds(pl.multiple_of(g * 16, 16), 16), 512 * k : 512 * k + 512] = jnp.concatenate(
                [u[i, 4 * k : 4 * k + 4] for i in range(4)], axis=0
            )

    first = lax.broadcasted_iota(jnp.int32, (2, 12, 8, D), 2) < SL

    outs = []
    for t in range(2):
        r = 12 * t
        if t == 0:
            for cp in (*backs, slab(0), slab(1)):
                cp.wait_recv()
        if t == 1:
            for cp in (slab(3), slab(2)):
                cp.wait_recv()
        att = ox[:, r : r + 12, 0:48, :].astype(F32)
        head = jnp.where(first, ic[:, r : r + 12].astype(F32), att[:, :, 0:8])
        att = jnp.concatenate([head, att[:, :, 8:48]], axis=2)
        res = (fx[:, r : r + 12, 0:48, :].astype(F32) + att).astype(BF).reshape(1152, D)
        xb[...] = norm(res, gain_m[...])
        acc = res.astype(F32)
        for k in range(4):
            pre = nt(xb[...], gat[1, k // 2, k % 2].reshape(512, D))
            hid = (0.5 * pre * (1.0 + lax.erf(pre * 0.7071067811865476))).astype(BF)
            acc = acc + nt(hid, w_d[:, 512 * k : 512 * k + 512])
        ob[t] = acc.astype(BF).reshape(2, 12, 48, D)
        cp = pltpu.make_async_copy(ob.at[t], out.at[:, pl.ds(r, 12)], osem.at[t])
        cp.start()
        outs.append(cp)

    for cp in (*steps.values(), *halos, *backs, *(slab(b) for b in range(4))):
        cp.wait_send()
    for cp in outs:
        cp.wait()


def body(fields, region, gain_attn, w_qkv, w_proj, gain_mlp, w_up, w_down):
    vm = pl.BlockSpec(memory_space=pltpu.VMEM)
    hbm = pl.BlockSpec(memory_space=pl.ANY)
    dma = pltpu.SemaphoreType.DMA
    out = pl.pallas_call(
        kernel,
        out_shape=jax.ShapeDtypeStruct((2, 24, 48, D), BF),
        in_specs=[vm, vm, vm, vm, hbm, hbm, vm, vm],
        out_specs=hbm,
        scratch_shapes=[
            pltpu.VMEM((3, 2, 2, 4, 2, 4, 16, D), BF),
            pltpu.VMEM((2, 27, 56, D), BF),
            pltpu.VMEM((2, 48, 48), jnp.int32),
            pltpu.VMEM((3 * D, D), BF),
            pltpu.VMEM((D, D), BF),
            pltpu.VMEM((D, FF), BF),
            pltpu.VMEM((2304, D), BF),
            pltpu.VMEM((1152, D), BF),
            pltpu.VMEM((2304, D), BF),
            pltpu.VMEM((2304, D), BF),
            pltpu.VMEM((2304, D), BF),
            pltpu.VMEM((16, WTOK, 128), F32),
            pltpu.VMEM((16, WTOK, 128), F32),
            pltpu.VMEM((576, D), BF),
            pltpu.VMEM((2, 27, 56, D), BF),
            pltpu.VMEM((2, 27, 8, D), BF),
            pltpu.VMEM((4, WTOK, 128), BF),
            pltpu.VMEM((128, 256), BF),
            pltpu.VMEM((128, 256), F32),
            pltpu.VMEM((512, 128), F32),
            pltpu.VMEM((2, 2, 12, 48, D), BF),
            dma((6, 13)),
            dma((6, 13)),
            dma((2,)),
            dma((6,)),
            dma((6,)),
            dma((6,)),
            dma((6,)),
            dma((4,)),
        ],
        compiler_params=pltpu.CompilerParams(
            collective_id=0, has_side_effects=True, vmem_limit_bytes=66 * 2**20 - 2**21
        ),
        name="block",
    )(
        w_qkv.T,
        w_proj.T,
        w_up.T,
        w_down.T,
        fields[0],
        region,
        gain_attn.reshape(1, D),
        gain_mlp.reshape(1, D),
    )
    return out[None]


def solution(mesh):
    in_specs = (
        P("mem", None, "lat", "lon", None),
        P("lat", "lon"),
        P(),
        P(None, ("mem", "lat", "lon")),
        P(None, ("mem", "lat", "lon")),
        P(),
        P(None, ("mem", "lat", "lon")),
        P(None, ("mem", "lat", "lon")),
    )
    out_specs = P("mem", None, "lat", "lon", None)
    return jax.shard_map(body, mesh=mesh, in_specs=in_specs, out_specs=out_specs, check_vma=False)
```
